32 devices in a mesh: dp: 8 (over z, x), mp: 4 (over y, core).
Axes of the slice: x: 2, y: 2, z: 4, core: 2. Of those that a mesh axis runs over, the one named last changes fastest.
Arguments:
- gradients: bfloat16 [8, 2, 4096, 1024], P('dp', None, None, 'mp'), may hold values from -6912 to 6912
- layer_mask: int32 [8, 2], P('dp'), may hold values from 0 to 1, as said below
- exit_losses: float32 [8, 2], P('dp'), may hold values from 1 to 24
- exit_weights: int32 [2], replicated, may hold values from 1 to 8
- params: float32 [2, 4096, 1024], P(None, 'dp', 'mp'), may hold values from -0.3 to 0.3
- moment: float32 [2, 4096, 1024], P(None, 'dp', 'mp'), may hold values from -6 to 6
- second: float32 [2, 4096, 1024], P(None, 'dp', 'mp'), may hold values from 0.5 to 4
Outputs:
- new_params: float32 [2, 4096, 1024], P(None, 'dp', 'mp')
- new_moment: float32 [2, 4096, 1024], P(None, 'dp', 'mp')
- new_second: float32 [2, 4096, 1024], P(None, 'dp', 'mp')
- exit_mean: float32 [2], replicated
The draws below stay inside these ranges and needn't reach their ends.
Inputs may be any that keep to these rules, and one draw needn't show every extreme that they name: `layer_mask`: every layer is run by at least one micro-batch.
All inputs are finite; a program needn't handle non-finite values.
Results may differ from the reference program's by a relative error of at most 0.0003.
Values sent between devices are 32-bit elements; how exact they have to be, the bound alone decides.
A program may use at most 64 MiB of HBM per device.

```python
import math
import jax
import jax.numpy as jnp
from jax import lax

D = 4096
KVW = 1024
LAYERS = 2
MB = 8


def draw_gradients(key, part):
    key_rows = jax.random.fold_in(key, 0)
    key_cols = jax.random.fold_in(key, 1)
    key_noise = jax.random.fold_in(key, 3)
    row_scale = jnp.exp(jax.random.uniform(key_rows, (D,), jnp.float32, math.log(0.3), math.log(3.0)))
    col_scale = jnp.exp(jax.random.uniform(key_cols, (KVW,), jnp.float32, math.log(0.3), math.log(3.0)))
    values = jax.random.normal(key_noise, (MB, LAYERS, D, KVW), jnp.float32)
    values = jnp.clip(values, -6.0, 6.0) * 128.0 * row_scale[:, None] * col_scale[None, :]
    return values.astype(jnp.bfloat16)


def draw_layer_mask(key, part):
    key_keep, key_force = jax.random.split(key)
    raw_draws = jax.random.randint(key_keep, (MB, LAYERS), 0, 1000)
    depth_index = jnp.arange(LAYERS, dtype=jnp.int32)
    threshold = 900 - 400 * depth_index // max(LAYERS - 1, 1)
    keep_flag = (raw_draws < threshold[None, :]).astype(jnp.int32)
    forced = jax.random.randint(key_force, (LAYERS,), 0, MB)
    row_index = jnp.arange(MB, dtype=jnp.int32)
    chosen = (row_index[:, None] == forced[None, :]).astype(jnp.int32)
    return jnp.maximum(keep_flag, chosen)


def draw_exit_losses(key, part):
    ramp = 1.0 + 2.0 * jnp.arange(MB, dtype=jnp.float32) / max(MB - 1, 1)
    base = jnp.exp(jax.random.uniform(key, (MB, LAYERS), jnp.float32, math.log(1.5), math.log(4.0)))
    return (ramp[:, None] * base).astype(jnp.float32)


def steps_of(stream_key, dims, cuts, smallest, high):
    level = 1.0
    for position, shards_of in cuts:
        heights = jax.random.uniform(jax.random.fold_in(jax.random.fold_in(stream_key, 6), position), (shards_of,), jnp.float32, smallest / len(cuts), high / len(cuts))
        level = level * jnp.repeat(jnp.exp(heights), dims[position] // shards_of).reshape((-1,) + (1,) * (len(dims) - 1 - position))
    return level


def gaussian(key, extent, scale, reach, shards=(), held_as=jnp.bfloat16):
    entries = scale * jax.random.normal(key, extent, jnp.float32)
    if shards:
        entries = entries * steps_of(key, extent, shards, -0.22, 0.18)
    return jnp.clip(entries, -reach, reach).astype(held_as)


def setup_inputs(seed: int = 0) -> dict:
    keys = jax.random.split(jax.random.key(seed), 8)
    gradients = draw_gradients(jax.random.fold_in(keys[7], 71), 0)
    layer_mask = draw_layer_mask(jax.random.fold_in(keys[7], 71), 0)
    exit_losses = draw_exit_losses(jax.random.fold_in(keys[7], 71), 0)
    exit_weights = jax.random.randint(keys[3], (LAYERS,), 1, 9).astype(jnp.int32)
    params = gaussian(keys[4], (LAYERS, D, KVW), 0.05, 0.3, ((1, 8), (2, 4)), jnp.float32)
    moment = gaussian(keys[5], (LAYERS, D, KVW), 1.0, 6.0, ((1, 8), (2, 4)), jnp.float32)
    second = jnp.clip(jnp.exp(math.log(4.0) - 2.0794415 * jax.random.uniform(keys[6], (LAYERS, D, KVW), jnp.float32) ** steps_of(keys[6], (LAYERS, D, KVW), ((1, 8), (2, 4)), -0.2, 0.2)), 0.5, 4.0)
    return dict(gradients=gradients, layer_mask=layer_mask, exit_losses=exit_losses, exit_weights=exit_weights, params=params, moment=moment, second=second)


max_rms = 1.0
eps_norm = 1e-06
eps_adam = 1e-08
beta_one = 0.9
beta_two = 0.95
learn_rate = 0.01
decay_rate = 0.1

def reference(gradients, layer_mask, exit_losses, exit_weights, params, moment, second):
    keep_float = layer_mask.astype(jnp.float32)
    layer_count = lax.optimization_barrier(jnp.sum(keep_float, axis=0))
    exit_mean = lax.optimization_barrier(jnp.sum(keep_float * exit_losses, axis=0)) / layer_count
    weight_float = exit_weights.astype(jnp.float32)
    weight_sum = jnp.sum(weight_float)

    def accumulate(running, pieces):
        block, keep_row = pieces
        return (running + block.astype(jnp.float32) * keep_row[:, None, None], None)
    summed, unused = lax.scan(accumulate, jnp.zeros((LAYERS, D, KVW), jnp.float32), (gradients, keep_float))
    factor_row = weight_float / (weight_sum * layer_count)
    gradient = summed * factor_row[:, None, None]
    rms_value = jnp.sqrt(jnp.sum(gradient * gradient) / (LAYERS * D * KVW))
    clip_scale = jnp.minimum(1.0, max_rms / (rms_value + eps_norm))
    clipped = clip_scale * gradient
    new_moment = beta_one * moment + (1.0 - beta_one) * clipped
    new_second = beta_two * second + (1.0 - beta_two) * clipped * clipped
    new_params = params - learn_rate * (new_moment / (jnp.sqrt(new_second) + eps_adam) + decay_rate * params)
    return (new_params, new_moment, new_second, exit_mean)
```

```python
import jax
import jax.numpy as jnp
from jax import lax
from jax.experimental import pallas as pl
from jax.experimental.pallas import tpu as pltpu
from jax.sharding import PartitionSpec as P

max_rms = 1.0
eps_norm = 1e-06
eps_adam = 1e-08
beta_one = 0.9
beta_two = 0.95
learn_rate = 0.01
decay_rate = 0.1

MESH_ID = pl.DeviceIdType.MESH
ROWS = 64
LANES = 128
LAG = 4
CHUNKS = 8
MINE, OTHER = 0, 1


def update(gradient, clip_scale, params, moment, second):
    clipped = clip_scale * gradient
    new_moment = beta_one * moment + (1.0 - beta_one) * clipped
    new_second = beta_two * second + (1.0 - beta_two) * clipped * clipped
    new_params = params - learn_rate * (
        new_moment / (jnp.sqrt(new_second) + eps_adam) + decay_rate * params
    )
    return new_params, new_moment, new_second


def any_mesh_body(entries, gradients, layer_mask, exit_losses, exit_weights, params, moment, second):
    keep_float = layer_mask[0].astype(jnp.float32)
    loss_terms = keep_float * exit_losses[0]
    local_term = gradients[0].astype(jnp.float32) * keep_float[:, None, None]
    summed = lax.psum_scatter(local_term, "dp", scatter_dimension=1, tiled=True)
    weight_float = exit_weights.astype(jnp.float32)
    weight_sum = jnp.sum(weight_float)
    layer_count, loss_sum = lax.psum((keep_float, loss_terms), "dp")
    gradient = summed * (weight_float / (weight_sum * layer_count))[:, None, None]
    square_sum = lax.psum(jnp.sum(gradient * gradient), ("dp", "mp"))
    rms_value = jnp.sqrt(square_sum / entries)
    clip_scale = jnp.minimum(1.0, max_rms / (rms_value + eps_norm))
    new = update(gradient, clip_scale, params, moment, second)
    return (*new, loss_sum / layer_count)


def line_kernel(
    n_mp, entries, mask_in, losses_in, weights_in, grads, params_in, moment_in, second_in,
    out, params_out, moment_out, second_out, stats_out, clip_out,
    mask, losses, weights, held, snd, xr, zr, ar, st0, st1, square,
    small_sem, load_sem, state_sem, send_sem, x_sem, z_sem, a_sem,
    st0_send, st0_recv, st1_send, st1_recv, y_in, x_in, end_in, middle_in, all_in,
):
    layers, rows = out.shape[0], out.shape[1]
    pieces = snd.shape[1]
    depth = snd.shape[2]
    per_layer = pieces // layers
    early = pieces // 2
    dp, mp = lax.axis_index("dp"), lax.axis_index("mp")
    z, x = dp // 2, lax.rem(dp, 2)
    upper = z // 2
    place = lax.rem(z + upper, 2)
    x_dev = z * 2 + 1 - x
    z_dev = (z + 1 - 2 * lax.rem(z, 2)) * 2 + x
    a_dev = (3 - z) * 2 + x

    barrier = pltpu.get_barrier_semaphore()
    devices = 8 * n_mp
    place_in_all = dp * n_mp + mp

    def away(i):
        other_z, other_x, other_mp = z ^ (i // (2 * n_mp)), x ^ (i // n_mp % 2), mp ^ (i % n_mp)
        other_dp = other_z * 2 + other_x
        return other_dp * n_mp + other_mp, {"dp": other_dp, "mp": other_mp}

    def greet(sem, device):
        pl.semaphore_signal(sem, inc=1, device_id=device, device_id_type=MESH_ID)

    for device in ({"dp": x_dev}, {"dp": z_dev}, {"mp": mp ^ 1}, {"mp": mp ^ 2}):
        greet(barrier, device)

    @pl.when(place == 1)
    def _():
        greet(barrier, {"dp": a_dev})

    small = [
        pltpu.make_async_copy(src, dst, small_sem.at[i])
        for i, (src, dst) in enumerate(((mask_in, mask), (losses_in, losses), (weights_in, weights)))
    ]
    for copy in small:
        copy.start()

    def load(slot, layer):
        k, side = slot // 2, slot % 2
        target = (k + upper * (3 - 2 * k)) * 2 + (x if side == MINE else 1 - x)
        return pltpu.make_async_copy(
            grads.at[0, layer, pl.ds(target * rows, rows), :], held.at[slot, layer], load_sem.at[slot, layer]
        )

    def fetch(*slots):
        for slot in slots:
            for layer in range(layers):
                load(slot, layer).start()

    def state():
        pairs = ((params_in, params_out), (moment_in, moment_out), (second_in, second_out))
        return [pltpu.make_async_copy(src, dst, state_sem.at[i]) for i, (src, dst) in enumerate(pairs)]

    fetch(7)
    pl.when(place == 0)(lambda: fetch(3))
    pl.when(place == 1)(lambda: fetch(1))

    def loaded(*slots):
        for slot in slots:
            for layer in range(layers):
                load(slot, layer).wait()

    for copy in small:
        copy.wait()
    lane = lax.broadcasted_iota(jnp.int32, st0.shape[1:], 1)
    tile = jnp.zeros(st0.shape[1:], jnp.float32)
    for layer in range(layers):
        keep = mask[0, layer].astype(jnp.float32)
        tile = jnp.where(lane == layer, keep, tile)
        tile = jnp.where(lane == layers + layer, keep * losses[0, layer], tile)
    st0[dp] = tile

    pl.when(place == 0)(lambda: pl.semaphore_wait(barrier, 4))
    pl.when(place == 1)(lambda: pl.semaphore_wait(barrier, 5))

    def meet():
        greet(y_in, {"mp": mp ^ 2})
        pl.semaphore_wait(y_in, 1)
        greet(x_in, {"dp": x_dev})
        pl.semaphore_wait(x_in, 1)

        @pl.when(place == 0)
        def _():
            greet(end_in, {"dp": z_dev})
            pl.semaphore_wait(all_in, 1)

        @pl.when(place == 1)
        def _():
            pl.semaphore_wait(end_in, 1)
            greet(middle_in, {"dp": a_dev})
            pl.semaphore_wait(middle_in, 1)
            greet(all_in, {"dp": z_dev})

    def own(slot, c):
        layer, r = c // per_layer, lax.rem(c, per_layer)
        keep = mask[0, layer].astype(jnp.float32)
        return held[slot, layer, pl.ds(pl.multiple_of(r * depth, depth), depth), :].astype(jnp.float32) * keep

    def push(slot, c, dst, sem, device):
        return pltpu.make_async_remote_copy(
            src_ref=snd.at[slot, c], dst_ref=dst, send_sem=send_sem.at[slot], recv_sem=sem,
            device_id={"dp": device}, device_id_type=MESH_ID,
        )

    def to_x(k, c):
        return push(2 * k + OTHER, c, xr.at[k, c], x_sem.at[k, c], x_dev)

    def to_z(slot, box, c):
        return push(slot, c, zr.at[box, c], z_sem.at[box, c], z_dev)

    def to_a(k, c):
        return push(2 * k + MINE, c, ar.at[3 - k, c], a_sem.at[3 - k, c], a_dev)

    def from_x(k, c):
        to_x(k, c).wait_recv()
        return xr[k, c]

    def from_z(box, c):
        to_z(0, box, c).wait_recv()
        return zr[box, c]

    def from_a(box, c):
        to_a(3 - box, c).wait_recv()
        return ar[box, c]

    def each(low, high, step):
        def one(c, carry):
            step(c)
            return carry

        lax.fori_loop(low, high, one, 0)

    def x_own(k, c):
        snd[2 * k + OTHER, c] = own(2 * k + OTHER, c)
        to_x(k, c).start()

    def share_stats(i):
        return pltpu.make_async_remote_copy(
            src_ref=st0.at[dp], dst_ref=st0.at[dp], send_sem=st0_send.at[i], recv_sem=st0_recv.at[dp],
            device_id={"dp": lax.rem(dp + i, 8)}, device_id_type=MESH_ID,
        )

    def stats_arrival(i):
        peer = lax.rem(dp + i, 8)
        return pltpu.make_async_remote_copy(
            src_ref=st0.at[dp], dst_ref=st0.at[peer], send_sem=st0_send.at[i], recv_sem=st0_recv.at[peer],
            device_id={"dp": peer}, device_id_type=MESH_ID,
        )

    @pl.when(place == 0)
    def _():
        loaded(7, 3)

        def first(c):
            x_own(3, c)

            @pl.when(c < early)
            def _():
                snd[3, c] = own(3, c)
                to_z(3, 0, c).start()

        each(0, 1, first)
        fetch(6, 5, 1, 4, 2, 0)
        each(1, pieces, first)
        meet()
        for copy in state():
            copy.start()
        loaded(1, 6, 5)
        for i in range(1, 8):
            share_stats(i).start()

        def second(c):
            snd[6, c] = own(6, c) + from_x(3, c)
            to_z(6, 3, c).start()
            x_own(2, c)

        each(0, pieces, second)
        loaded(4, 2, 0)

        def send_own_level(c):
            snd[1, c] = own(1, c) + from_z(1, c)
            to_x(0, c).start()

        def third(c):
            snd[4, c] = own(4, c) + from_x(2, c)
            to_z(4, 2, c).start()

        def third_a(c):
            third(c)
            x_own(1, c + early)

        def third_b(c):
            third(c)
            send_own_level(c - (pieces - early))

        each(0, pieces - early, third_a)
        each(pieces - early, pieces, third_b)

        def fourth(c):
            snd[2, c] = own(2, c) + from_x(1, c)
            to_z(2, 1, c).start()
            send_own_level(c)

        each(early, pieces, fourth)

        def fifth(c):
            snd[2, c] = own(2, c)
            to_z(2, 1, c).start()

        each(0, early, fifth)

    @pl.when(place == 1)
    def _():
        loaded(7, 1)

        def first(c):
            x_own(3, c)
            snd[1, c] = own(1, c)
            to_z(1, 1, c).start()

        each(0, 1, first)
        fetch(6, 5, 3, 4, 2, 0)
        each(1, pieces, first)
        meet()
        for copy in state():
            copy.start()
        loaded(3, 6, 5)
        for i in range(1, 8):
            share_stats(i).start()
        loaded(4, 2, 0)

        def pass_out(c):
            snd[0, c] = own(0, c) + from_a(0, c)
            to_z(0, 0, c).start()

        def second(c):
            x_own(2, c)
            snd[6, c] = own(6, c) + from_x(3, c) + from_z(3, c)
            to_a(3, c).start()

        def second_b(c):
            second(c)
            pass_out(c - LAG)

        each(0, LAG, second)
        each(LAG, pieces, second_b)

        def third(c):
            snd[4, c] = own(4, c) + from_x(2, c) + from_z(2, c)
            to_a(2, c).start()

        def third_a(c):
            x_own(1, c + early)
            third(c)

            @pl.when(c < LAG)
            def _():
                pass_out(c + pieces - LAG)

        def third_b(c):
            late = c - (pieces - early)
            snd[3, late] = own(3, late) + from_z(0, late)
            to_x(1, late).start()
            third(c)

        each(0, pieces - early, third_a)
        each(pieces - early, pieces, third_b)

    for i in range(1, 8):
        stats_arrival(i).wait_recv()
    total = st0[0]
    for i in range(1, 8):
        total = total + st0[i]
    stats_out[...] = total
    weight_sum = weights[0].astype(jnp.float32)
    for layer in range(1, layers):
        weight_sum = weight_sum + weights[layer].astype(jnp.float32)
    square[...] = jnp.zeros_like(square)
    factors = [weights[layer].astype(jnp.float32) / (weight_sum * total[:, layer : layer + 1]) for layer in range(layers)]

    def finish(layer, c, summed):
        factor = factors[layer]
        gradient = summed * factor
        r = lax.rem(c, per_layer)
        out[layer, pl.ds(pl.multiple_of(r * depth, depth), depth), :] = gradient
        squares = gradient * gradient
        square[...] += jnp.sum(squares.reshape(depth // 8, 8, squares.shape[1]), axis=0)

    @pl.when(place == 0)
    def _():
        for layer in range(layers):
            def last(c, layer=layer):
                finish(layer, c, own(0, c) + from_z(0, c) + from_x(0, c))

            each(layer * per_layer, (layer + 1) * per_layer, last)

    @pl.when(place == 1)
    def _():
        for layer in list(range(layers))[::-1]:
            def last(c, layer=layer):
                finish(layer, c, own(2, c) + from_x(1, c) + from_a(1, c) + from_z(1, c))

            each(layer * per_layer, (layer + 1) * per_layer, last)

    def share_square(i):
        return pltpu.make_async_remote_copy(
            src_ref=st1.at[place_in_all], dst_ref=st1.at[place_in_all],
            send_sem=st1_send.at[i], recv_sem=st1_recv.at[place_in_all],
            device_id=away(i)[1], device_id_type=MESH_ID,
        )

    def square_arrival(i):
        peer, device = away(i)
        return pltpu.make_async_remote_copy(
            src_ref=st1.at[place_in_all], dst_ref=st1.at[peer], send_sem=st1_send.at[i], recv_sem=st1_recv.at[peer],
            device_id=device, device_id_type=MESH_ID,
        )

    for copy in state():
        copy.wait()
    folded = jnp.sum(square[...], axis=0, keepdims=True)
    st1[place_in_all] = sum(folded[:, i : i + LANES] for i in range(0, folded.shape[1], LANES))
    for i in range(devices - 1, 0, -1):
        share_square(i).start()
    for i in range(1, devices):
        square_arrival(i).wait_recv()
    all_rows = st1[0]
    for i in range(1, devices):
        all_rows = all_rows + st1[i]
    square_sum = jnp.sum(all_rows, keepdims=True)
    rms_value = jnp.sqrt(square_sum / entries)
    clip_out[...] = jnp.broadcast_to(jnp.minimum(1.0, max_rms / (rms_value + eps_norm)), clip_out.shape)

    for i in range(1, 8):
        share_stats(i).wait_send()
    for i in range(1, devices):
        share_square(i).wait_send()

    def sent(slot):
        pltpu.make_async_remote_copy(
            src_ref=snd.at[slot], dst_ref=zr.at[0], send_sem=send_sem.at[slot], recv_sem=z_sem.at[0, 0],
            device_id={"dp": z_dev}, device_id_type=MESH_ID,
        ).wait_send()

    for slot in range(1, 8):
        if slot != 2:
            sent(slot)

    pl.when(place == 0)(lambda: sent(2))
    pl.when(place == 1)(lambda: sent(0))


def update_kernel(gradient, params, moment, second, stats, clip, params_out, moment_out, second_out, mean_out, news, sem):
    layers, rows = gradient.shape[0], gradient.shape[1]
    outs = (params_out, moment_out, second_out)
    depth = rows * layers // CHUNKS
    per_layer = rows // depth

    def put(i, layer, part):
        window = (layer, pl.ds(part * depth, depth))
        return pltpu.make_async_copy(news.at[(i, *window)], outs[i].at[window], sem.at[i, layer, part])

    chunks = [(layer, part) for layer in range(layers) for part in range(per_layer)]
    for layer, part in chunks:
        window = (layer, pl.ds(part * depth, depth))
        new = update(gradient[window], clip[...], params[window], moment[window], second[window])
        for i in range(3):
            news[(i, *window)] = new[i]
            put(i, layer, part).start()
    mean_out[...] = stats[:, layers : 2 * layers] / stats[:, :layers]
    for layer, part in chunks:
        for i in range(3):
            put(i, layer, part).wait()


def line_body(n_mp, entries, gradients, layer_mask, exit_losses, exit_weights, params, moment, second):
    layers, rows, columns = params.shape
    depth = min(ROWS, rows)
    pieces = layers * (rows // depth)
    vmem, hbm = pl.BlockSpec(memory_space=pltpu.VMEM), pl.BlockSpec(memory_space=pltpu.HBM)
    block = (pieces, depth, columns)
    f32, dma, regular = jnp.float32, pltpu.SemaphoreType.DMA, pltpu.SemaphoreType.REGULAR
    state = jax.ShapeDtypeStruct((layers, rows, columns), f32)

    def kernel(*refs):
        line_kernel(n_mp, entries, *refs)

    *held, stats, clip = pl.pallas_call(
        kernel,
        name="line_reduce",
        out_shape=(
            state, state, state, state,
            jax.ShapeDtypeStruct((1, LANES), f32),
            jax.ShapeDtypeStruct((1, columns), f32),
        ),
        in_specs=[hbm] * 7,
        out_specs=[vmem] * 6,
        scratch_shapes=[
            pltpu.SMEM(layer_mask.shape, layer_mask.dtype),
            pltpu.SMEM(exit_losses.shape, exit_losses.dtype),
            pltpu.SMEM(exit_weights.shape, exit_weights.dtype),
            pltpu.VMEM((8, layers, rows, columns), gradients.dtype),
            pltpu.VMEM((8, *block), f32),
            pltpu.VMEM((4, *block), f32),
            pltpu.VMEM((4, *block), f32),
            pltpu.VMEM((2, *block), f32),
            pltpu.VMEM((8, 1, LANES), f32),
            pltpu.VMEM((8 * n_mp, 1, LANES), f32),
            pltpu.VMEM((8, columns), f32),
            dma((3,)), dma((8, layers)), dma((3,)), dma((8,)), dma((4, pieces)), dma((4, pieces)), dma((2, pieces)),
            dma((8,)), dma((8,)), dma((8 * n_mp,)), dma((8 * n_mp,)), regular, regular, regular, regular, regular,
        ],
        compiler_params=pltpu.CompilerParams(
            collective_id=0, has_side_effects=True, vmem_limit_bytes=40 * 1024 * 1024
        ),
    )(*(
        pltpu.with_memory_space_constraint(a, pltpu.HBM)
        for a in (layer_mask, exit_losses, exit_weights, gradients, params, moment, second)
    ))
    *new, mean = pl.pallas_call(
        update_kernel,
        name="update",
        out_shape=(state, state, state, jax.ShapeDtypeStruct((1, layers), f32)),
        in_specs=[vmem] * 6,
        out_specs=(hbm, hbm, hbm, vmem),
        scratch_shapes=[pltpu.VMEM((3, layers, rows, columns), f32), dma((3, layers, CHUNKS // layers))],
        compiler_params=pltpu.CompilerParams(vmem_limit_bytes=16 * 1024 * 1024),
    )(*held, stats, clip)
    return (*new, mean[0])


def solution(mesh):
    state = P(None, "dp", "mp")
    placed = (P("dp", None, None, "mp"), P("dp", None), P("dp", None), P(), state, state, state)
    n_dp, n_mp = mesh.shape["dp"], mesh.shape["mp"]

    def whole(*args):
        entries = args[4].size
        layers = args[4].shape[0]

        def body(*blocks):
            if n_dp == 8 and n_mp == 4 and layers == 2:
                return line_body(n_mp, entries, *blocks)
            return any_mesh_body(entries, *blocks)

        return jax.shard_map(
            body, mesh=mesh, in_specs=placed, out_specs=(state, state, state, P()), check_vma=False
        )(*args)

    return whole
```

```python
import jax
import jax.numpy as jnp
from jax import lax
from jax.experimental import pallas as pl
from jax.experimental.pallas import tpu as pltpu
from jax.sharding import PartitionSpec as P

max_rms = 1.0
eps_norm = 1e-06
eps_adam = 1e-08
beta_one = 0.9
beta_two = 0.95
learn_rate = 0.01
decay_rate = 0.1

MESH_ID = pl.DeviceIdType.MESH
ROWS = 64
LANES = 128
LAG = 4
EARLY = 10
TAIL = 6
START = 11
PACED = 4
CHUNK = 256
STEP = 32
MINE, OTHER = 0, 1


def update(gradient, clip_scale, params, moment, second):
    clipped = clip_scale * gradient
    new_moment = beta_one * moment + (1.0 - beta_one) * clipped
    new_second = beta_two * second + (1.0 - beta_two) * clipped * clipped
    new_params = params - learn_rate * (
        new_moment / (jnp.sqrt(new_second) + eps_adam) + decay_rate * params
    )
    return new_params, new_moment, new_second


def any_mesh_body(entries, gradients, layer_mask, exit_losses, exit_weights, params, moment, second):
    keep_float = layer_mask[0].astype(jnp.float32)
    loss_terms = keep_float * exit_losses[0]
    local_term = gradients[0].astype(jnp.float32) * keep_float[:, None, None]
    summed = lax.psum_scatter(local_term, "dp", scatter_dimension=1, tiled=True)
    weight_float = exit_weights.astype(jnp.float32)
    weight_sum = jnp.sum(weight_float)
    layer_count, loss_sum = lax.psum((keep_float, loss_terms), "dp")
    gradient = summed * (weight_float / (weight_sum * layer_count))[:, None, None]
    square_sum = lax.psum(jnp.sum(gradient * gradient), ("dp", "mp"))
    rms_value = jnp.sqrt(square_sum / entries)
    clip_scale = jnp.minimum(1.0, max_rms / (rms_value + eps_norm))
    new = update(gradient, clip_scale, params, moment, second)
    return (*new, loss_sum / layer_count)


def line_kernel(
    n_mp, entries, mask_in, losses_in, weights_in, grads, params_in, moment_in, second_in,
    out, params_out, moment_out, second_out, stats_out, clip_out,
    mask, losses, weights, held, snd, xr, zr, ar, tr, st0, st1, square,
    small_sem, load_sem, state_sem, send_sem, x_sem, z_sem, a_sem, t_sem,
    st0_send, st0_recv, st1_send, st1_recv, y_in, x_in, end_in, middle_in, all_in,
):
    layers, rows = out.shape[0], out.shape[1]
    pieces = snd.shape[1]
    depth = snd.shape[2]
    per_layer = pieces // layers
    early, tail = EARLY, EARLY - TAIL
    small = [
        pltpu.make_async_copy(src, dst, small_sem.at[i])
        for i, (src, dst) in enumerate(((mask_in, mask), (losses_in, losses), (weights_in, weights)))
    ]
    for copy in small:
        copy.start()

    dp, mp = lax.axis_index("dp"), lax.axis_index("mp")
    z, x = dp // 2, lax.rem(dp, 2)
    upper = z // 2
    place = lax.rem(z + upper, 2)
    x_dev = z * 2 + 1 - x
    z_dev = (z + 1 - 2 * lax.rem(z, 2)) * 2 + x
    a_dev = (3 - z) * 2 + x

    barrier = pltpu.get_barrier_semaphore()
    devices = 8 * n_mp
    place_in_all = dp * n_mp + mp

    def away(i):
        other_z, other_x, other_mp = z ^ (i // (2 * n_mp)), x ^ (i // n_mp % 2), mp ^ (i % n_mp)
        other_dp = other_z * 2 + other_x
        return other_dp * n_mp + other_mp, {"dp": other_dp, "mp": other_mp}

    def greet(sem, device):
        pl.semaphore_signal(sem, inc=1, device_id=device, device_id_type=MESH_ID)

    def load(slot, layer):
        k, side = slot // 2, slot % 2
        target = (k + upper * (3 - 2 * k)) * 2 + (x if side == MINE else 1 - x)
        return pltpu.make_async_copy(
            grads.at[0, layer, pl.ds(target * rows, rows), :], held.at[slot, layer], load_sem.at[slot, layer]
        )

    def fetch(*slots):
        for slot in slots:
            for layer in range(layers):
                load(slot, layer).start()

    def state():
        pairs = ((params_in, params_out), (moment_in, moment_out), (second_in, second_out))
        return [pltpu.make_async_copy(src, dst, state_sem.at[i]) for i, (src, dst) in enumerate(pairs)]

    load(7, 0).start()
    for device in ({"dp": x_dev}, {"dp": z_dev}, {"mp": mp ^ 1}, {"mp": mp ^ 2}):
        greet(barrier, device)

    @pl.when(place == 1)
    def _():
        greet(barrier, {"dp": a_dev})

    load(7, 1).start()
    pl.when(place == 0)(lambda: fetch(3))
    pl.when(place == 1)(lambda: fetch(1))

    def loaded(*slots):
        for slot in slots:
            for layer in range(layers):
                load(slot, layer).wait()

    for copy in small:
        copy.wait()
    lane = lax.broadcasted_iota(jnp.int32, st0.shape[1:], 1)
    tile = jnp.zeros(st0.shape[1:], jnp.float32)
    for layer in range(layers):
        keep = mask[0, layer].astype(jnp.float32)
        tile = jnp.where(lane == layer, keep, tile)
        tile = jnp.where(lane == layers + layer, keep * losses[0, layer], tile)
    st0[dp] = tile

    pl.when(place == 0)(lambda: pl.semaphore_wait(barrier, 4))
    pl.when(place == 1)(lambda: pl.semaphore_wait(barrier, 5))

    def meet():
        greet(y_in, {"mp": mp ^ 2})
        pl.semaphore_wait(y_in, 1)
        greet(x_in, {"dp": x_dev})
        pl.semaphore_wait(x_in, 1)

        @pl.when(place == 0)
        def _():
            greet(end_in, {"dp": z_dev})
            pl.semaphore_wait(all_in, 1)

        @pl.when(place == 1)
        def _():
            pl.semaphore_wait(end_in, 1)
            greet(middle_in, {"dp": a_dev})
            pl.semaphore_wait(middle_in, 1)
            greet(all_in, {"dp": z_dev})

    def own(slot, c):
        layer, r = c // per_layer, lax.rem(c, per_layer)
        keep = mask[0, layer].astype(jnp.float32)
        return held[slot, layer, pl.ds(pl.multiple_of(r * depth, depth), depth), :].astype(jnp.float32) * keep

    def push(slot, c, dst, sem, device):
        return pltpu.make_async_remote_copy(
            src_ref=snd.at[slot, c], dst_ref=dst, send_sem=send_sem.at[slot], recv_sem=sem,
            device_id={"dp": device}, device_id_type=MESH_ID,
        )

    def to_x(k, c):
        return push(2 * k + OTHER, c, xr.at[k, c], x_sem.at[k, c], x_dev)

    def to_z(slot, box, c):
        return push(slot, c, zr.at[box, c], z_sem.at[box, c], z_dev)

    def to_a(k, c):
        return push(2 * k + MINE, c, ar.at[3 - k, c], a_sem.at[3 - k, c], a_dev)

    def to_tail(c):
        return push(2, c, tr.at[c - tail], t_sem.at[c - tail], z_dev)

    def from_tail(c):
        to_tail(c).wait_recv()
        return tr[c - tail]

    def from_x(k, c):
        to_x(k, c).wait_recv()
        return xr[k, c]

    def from_z(box, c):
        to_z(0, box, c).wait_recv()
        return zr[box, c]

    def from_a(box, c):
        to_a(3 - box, c).wait_recv()
        return ar[box, c]

    def each(low, high, step):
        def one(c, carry):
            step(c)
            return carry

        lax.fori_loop(low, high, one, 0)

    def x_own(k, c):
        snd[2 * k + OTHER, c] = own(2 * k + OTHER, c)
        to_x(k, c).start()

    def share_stats(i):
        return pltpu.make_async_remote_copy(
            src_ref=st0.at[dp], dst_ref=st0.at[dp], send_sem=st0_send.at[i], recv_sem=st0_recv.at[dp],
            device_id={"dp": lax.rem(dp + i, 8)}, device_id_type=MESH_ID,
        )

    def stats_arrival(i):
        peer = lax.rem(dp + i, 8)
        return pltpu.make_async_remote_copy(
            src_ref=st0.at[dp], dst_ref=st0.at[peer], send_sem=st0_send.at[i], recv_sem=st0_recv.at[peer],
            device_id={"dp": peer}, device_id_type=MESH_ID,
        )

    @pl.when(place == 0)
    def _():
        load(7, 0).wait()
        x_own(3, 0)
        load(7, 1).wait()
        loaded(3)

        def first(c):
            @pl.when(c > 0)
            def _():
                x_own(3, c)

            @pl.when(c < early)
            def _():
                snd[3, c] = own(3, c)
                to_z(3, 0, c).start()

        each(0, 1, first)
        fetch(6, 5, 1, 4, 2, 0)
        each(1, pieces, first)
        meet()
        for copy in state():
            copy.start()
        loaded(1, 6, 5)
        for i in range(1, 8):
            share_stats(i).start()

        def second(c):
            snd[6, c] = own(6, c) + from_x(3, c)
            to_z(6, 3, c).start()
            x_own(2, c)

        each(0, pieces, second)
        loaded(4, 2, 0)

        def send_own_level(c):
            snd[1, c] = own(1, c) + from_z(1, c)
            to_x(0, c).start()

        def third(c):
            snd[4, c] = own(4, c) + from_x(2, c)
            to_z(4, 2, c).start()

        def third_a(c):
            third(c)
            x_own(1, c + early)

        def third_b(c):
            third(c)
            send_own_level(c - (pieces - early))

        each(0, pieces - early, third_a)
        each(pieces - early, pieces, third_b)

        def fourth(c):
            snd[2, c] = own(2, c) + from_x(1, c)
            to_z(2, 1, c).start()
            send_own_level(c)

        each(early, pieces, fourth)

        def fifth(c):
            snd[2, c] = own(2, c)
            to_z(2, 1, c).start()

        each(0, tail, fifth)

    @pl.when(place == 1)
    def _():
        load(7, 0).wait()
        x_own(3, 0)
        load(7, 1).wait()
        loaded(1)

        def first(c):
            @pl.when(c > 0)
            def _():
                x_own(3, c)

            snd[1, c] = own(1, c)
            to_z(1, 1, c).start()

        each(0, 1, first)
        fetch(6, 5, 3, 4, 2, 0)
        each(1, pieces, first)
        meet()
        for copy in state():
            copy.start()
        loaded(3, 6, 5)
        for i in range(1, 8):
            share_stats(i).start()
        loaded(4, 2, 0)

        def pass_out(c):
            snd[0, c] = own(0, c) + from_a(0, c)
            to_z(0, 0, c).start()

        def second(c):
            x_own(2, c)

            @pl.when(c < early)
            def _():
                snd[3, c] = own(3, c) + from_z(0, c)
                to_x(1, c).start()

            snd[6, c] = own(6, c) + from_x(3, c) + from_z(3, c)
            to_a(3, c).start()

        def second_b(c):
            second(c)
            pass_out(c - LAG)

        each(0, LAG, second)
        each(LAG, pieces, second_b)

        def third(c):
            @pl.when(c < pieces - early)
            def _():
                x_own(1, c + early)

            snd[4, c] = own(4, c) + from_x(2, c) + from_z(2, c)
            to_a(2, c).start()

            @pl.when(c < LAG)
            def _():
                pass_out(c + pieces - LAG)

        def return_tail(c):
            snd[2, c] = own(2, c) + from_x(1, c) + from_a(1, c)
            to_tail(c).start()

        def third_b(c):
            third(c)
            return_tail(c - LAG)

        each(0, tail + LAG, third)
        each(tail + LAG, early + LAG, third_b)
        each(early + LAG, pieces, third)

    for copy in state():
        copy.wait()
    def weigh(ref, layer, c, factor):
        window = (layer, pl.ds(pl.multiple_of(c * depth, depth), depth))
        ref[window] = ref[window] * factor

    for layer in range(layers):
        def weigh_all(c, layer=layer):
            weigh(params_out, layer, c, 1.0 - learn_rate * decay_rate)
            weigh(moment_out, layer, c, beta_one)
            weigh(second_out, layer, c, beta_two)

        each(0, per_layer, weigh_all)

    for i in range(1, 8):
        stats_arrival(i).wait_recv()
    total = st0[0]
    for i in range(1, 8):
        total = total + st0[i]
    stats_out[...] = total
    weight_sum = weights[0].astype(jnp.float32)
    for layer in range(1, layers):
        weight_sum = weight_sum + weights[layer].astype(jnp.float32)
    square[...] = jnp.zeros_like(square)
    factors = [weights[layer].astype(jnp.float32) / (weight_sum * total[:, layer : layer + 1]) for layer in range(layers)]

    def count(gradient):
        squares = gradient * gradient
        square[...] += jnp.sum(squares.reshape(depth // 8, 8, squares.shape[1]), axis=0)

    def finish(layer, c, summed):
        gradient = summed * factors[layer]
        r = lax.rem(c, per_layer)
        out[layer, pl.ds(pl.multiple_of(r * depth, depth), depth), :] = gradient
        return gradient

    def spans(low, high):
        cuts = [low, *(b for b in range(per_layer, pieces, per_layer) if low < b < high), high]
        return [(a // per_layer, a, b) for a, b in zip(cuts, cuts[1:]) if a < b]

    def last(c, layer):
        return finish(layer, c, own(2, c) + from_x(1, c) + from_a(1, c) + from_z(1, c))

    def finish_only(c, layer):
        finish(layer, c, snd[2, c] + from_z(1, c))

    def last_end(c, layer):
        count(finish(layer, c, own(0, c) + from_z(0, c) + from_x(0, c)))

    def count_tail(c, layer):
        snd[2, c] = own(2, c)
        count((snd[2, c] + from_tail(c)) * factors[layer])

    def paced(c, layer):
        to_z(2, 1, c - START + tail).start()
        last_end(c, layer)

    def over(step, *ranges):
        for low, high in ranges:
            for layer, a, b in spans(low, high):
                each(a, b, lambda c, layer=layer: step(c, layer))

    @pl.when(place == 0)
    def _():
        over(count_tail, (tail, early))
        over(last_end, (0, START))
        over(paced, (START, START + PACED))
        over(last_end, (START + PACED, pieces))

    @pl.when(place == 1)
    def _():
        over(lambda c, layer: count(last(c, layer)), (early, pieces), (0, tail))

    def share_square(i):
        return pltpu.make_async_remote_copy(
            src_ref=st1.at[place_in_all], dst_ref=st1.at[place_in_all],
            send_sem=st1_send.at[i], recv_sem=st1_recv.at[place_in_all],
            device_id=away(i)[1], device_id_type=MESH_ID,
        )

    def square_arrival(i):
        peer, device = away(i)
        return pltpu.make_async_remote_copy(
            src_ref=st1.at[place_in_all], dst_ref=st1.at[peer], send_sem=st1_send.at[i], recv_sem=st1_recv.at[peer],
            device_id=device, device_id_type=MESH_ID,
        )

    folded = jnp.sum(square[...], axis=0, keepdims=True)
    st1[place_in_all] = sum(folded[:, i : i + LANES] for i in range(0, folded.shape[1], LANES))
    for i in range(devices - 1, 0, -1):
        share_square(i).start()

    @pl.when(place == 0)
    def _():
        each(tail + PACED, early, lambda c: to_z(2, 1, c).start())

    @pl.when(place == 1)
    def _():
        over(finish_only, (tail, early))

    for i in range(1, devices):
        square_arrival(i).wait_recv()
    all_rows = st1[0]
    for i in range(1, devices):
        all_rows = all_rows + st1[i]
    square_sum = jnp.sum(all_rows, keepdims=True)
    rms_value = jnp.sqrt(square_sum / entries)
    clip_out[...] = jnp.broadcast_to(jnp.minimum(1.0, max_rms / (rms_value + eps_norm)), clip_out.shape)

    for i in range(1, 8):
        share_stats(i).wait_send()
    for i in range(1, devices):
        share_square(i).wait_send()

    def sent(slot, low=0, high=pieces):
        pltpu.make_async_remote_copy(
            src_ref=snd.at[slot, pl.ds(low, high - low)], dst_ref=zr.at[0, pl.ds(low, high - low)],
            send_sem=send_sem.at[slot], recv_sem=z_sem.at[0, 0],
            device_id={"dp": z_dev}, device_id_type=MESH_ID,
        ).wait_send()

    for slot in (1, 3, 4, 5, 6, 7):
        sent(slot)

    @pl.when(place == 0)
    def _():
        sent(2)

    @pl.when(place == 1)
    def _():
        sent(0)
        sent(2, tail, early)


def update_kernel(gradient, params, moment, second, stats, clip, params_out, moment_out, second_out, mean_out, news, mean, sem, mean_sem):
    layers, rows = gradient.shape[0], gradient.shape[1]
    outs = (params_out, moment_out, second_out)
    chunk, step = min(CHUNK, rows), min(STEP, rows)
    mean[...] = stats[:, layers : 2 * layers] / stats[:, :layers]
    mean_copy = pltpu.make_async_copy(mean, mean_out, mean_sem)
    mean_copy.start()
    clip_scale = clip[...]
    first_scale = (1.0 - beta_one) * clip_scale
    second_scale = (1.0 - beta_two) * clip_scale * clip_scale

    def put(i, layer, low):
        window = (layer, pl.ds(low, chunk))
        return pltpu.make_async_copy(news.at[(i, *window)], outs[i].at[window], sem.at[i])

    chunks = [(layer, low) for layer in range(layers) for low in range(0, rows, chunk)]
    for layer, low in chunks:
        for start in range(low, low + chunk, step):
            window = (layer, pl.ds(start, step))
            held = gradient[window]
            new_moment = moment[window] + first_scale * held
            new_second = second[window] + second_scale * (held * held)
            root = new_second * lax.rsqrt(new_second)
            news[(0, *window)] = params[window] - learn_rate * (new_moment / (root + eps_adam))
            news[(1, *window)] = new_moment
            news[(2, *window)] = new_second
        for i in range(3):
            put(i, layer, low).start()
    for i in range(3):
        pltpu.make_async_copy(news.at[i], outs[i], sem.at[i]).wait()
    mean_copy.wait()


def line_body(n_mp, entries, gradients, layer_mask, exit_losses, exit_weights, params, moment, second):
    layers, rows, columns = params.shape
    depth = min(ROWS, rows)
    pieces = layers * (rows // depth)
    vmem, hbm = pl.BlockSpec(memory_space=pltpu.VMEM), pl.BlockSpec(memory_space=pltpu.HBM)
    block = (pieces, depth, columns)
    f32, dma, regular = jnp.float32, pltpu.SemaphoreType.DMA, pltpu.SemaphoreType.REGULAR
    state = jax.ShapeDtypeStruct((layers, rows, columns), f32)

    def kernel(*refs):
        pl.run_scoped(lambda *sems: line_kernel(n_mp, entries, *refs, *sems),
            dma((3,)), dma((8, layers)), dma((3,)), dma((8,)), dma((4, pieces)), dma((4, pieces)), dma((2, pieces)), dma((TAIL,)),
            dma((8,)), dma((8,)), dma((8 * n_mp,)), dma((8 * n_mp,)), regular, regular, regular, regular, regular,
        )

    *held, stats, clip = pl.pallas_call(
        kernel,
        name="line_reduce",
        out_shape=(
            state, state, state, state,
            jax.ShapeDtypeStruct((1, LANES), f32),
            jax.ShapeDtypeStruct((1, columns), f32),
        ),
        in_specs=[hbm] * 7,
        out_specs=[vmem] * 6,
        scratch_shapes=[
            pltpu.SMEM(layer_mask.shape, layer_mask.dtype),
            pltpu.SMEM(exit_losses.shape, exit_losses.dtype),
            pltpu.SMEM(exit_weights.shape, exit_weights.dtype),
            pltpu.VMEM((8, layers, rows, columns), gradients.dtype),
            pltpu.VMEM((8, *block), f32),
            pltpu.VMEM((4, *block), f32),
            pltpu.VMEM((4, *block), f32),
            pltpu.VMEM((2, *block), f32),
            pltpu.VMEM((TAIL, *block[1:]), f32),
            pltpu.VMEM((8, 1, LANES), f32),
            pltpu.VMEM((8 * n_mp, 1, LANES), f32),
            pltpu.VMEM((8, columns), f32),
        ],
        compiler_params=pltpu.CompilerParams(
            collective_id=0, has_side_effects=True, vmem_limit_bytes=40 * 1024 * 1024
        ),
    )(*(
        pltpu.with_memory_space_constraint(a, pltpu.HBM)
        for a in (layer_mask, exit_losses, exit_weights, gradients, params, moment, second)
    ))
    *new, mean = pl.pallas_call(
        update_kernel,
        name="update",
        out_shape=(state, state, state, jax.ShapeDtypeStruct((1, layers), f32)),
        in_specs=[vmem] * 6,
        out_specs=[hbm] * 4,
        scratch_shapes=[pltpu.VMEM((3, layers, rows, columns), f32), pltpu.VMEM((1, layers), f32), dma((3,)), dma],
        compiler_params=pltpu.CompilerParams(vmem_limit_bytes=16 * 1024 * 1024),
    )(*held, stats, clip)
    return (*new, mean[0])


def solution(mesh):
    state = P(None, "dp", "mp")
    placed = (P("dp", None, None, "mp"), P("dp", None), P("dp", None), P(), state, state, state)
    n_dp, n_mp = mesh.shape["dp"], mesh.shape["mp"]

    def whole(*args):
        entries = args[4].size
        layers = args[4].shape[0]

        def body(*blocks):
            if n_dp == 8 and n_mp == 4 and layers == 2:
                return line_body(n_mp, entries, *blocks)
            return any_mesh_body(entries, *blocks)

        return jax.shard_map(
            body, mesh=mesh, in_specs=placed, out_specs=(state, state, state, P()), check_vma=False
        )(*args)

    return whole
```

```python
import jax
import jax.numpy as jnp
from jax import lax
from jax.experimental import pallas as pl
from jax.experimental.pallas import tpu as pltpu
from jax.sharding import PartitionSpec as P

max_rms = 1.0
eps_norm = 1e-06
eps_adam = 1e-08
beta_one = 0.9
beta_two = 0.95
learn_rate = 0.01
decay_rate = 0.1

MESH_ID = pl.DeviceIdType.MESH
ROWS = 32
LANES = 128
LAG = 8
EARLY = (18, 21)
START = (18, 24)
PACED = (11, 5)
TAIL = 13
CHUNK = 64
STEP = 32
MINE, OTHER = 0, 1


def update(gradient, clip_scale, params, moment, second):
    clipped = clip_scale * gradient
    new_moment = beta_one * moment + (1.0 - beta_one) * clipped
    new_second = beta_two * second + (1.0 - beta_two) * clipped * clipped
    new_params = params - learn_rate * (
        new_moment / (jnp.sqrt(new_second) + eps_adam) + decay_rate * params
    )
    return new_params, new_moment, new_second


def any_mesh_body(entries, gradients, layer_mask, exit_losses, exit_weights, params, moment, second):
    keep_float = layer_mask[0].astype(jnp.float32)
    loss_terms = keep_float * exit_losses[0]
    local_term = gradients[0].astype(jnp.float32) * keep_float[:, None, None]
    summed = lax.psum_scatter(local_term, "dp", scatter_dimension=1, tiled=True)
    weight_float = exit_weights.astype(jnp.float32)
    weight_sum = jnp.sum(weight_float)
    layer_count, loss_sum = lax.psum((keep_float, loss_terms), "dp")
    gradient = summed * (weight_float / (weight_sum * layer_count))[:, None, None]
    square_sum = lax.psum(jnp.sum(gradient * gradient), ("dp", "mp"))
    rms_value = jnp.sqrt(square_sum / entries)
    clip_scale = jnp.minimum(1.0, max_rms / (rms_value + eps_norm))
    new = update(gradient, clip_scale, params, moment, second)
    return (*new, loss_sum / layer_count)


def line_kernel(
    n_mp, entries, mask_in, losses_in, weights_in, grads, params_in, moment_in, second_in,
    out, params_out, moment_out, second_out, stats_out, clip_out,
    mask, losses, weights, held, snd, xr, zr, ar, tr, st0, st1, square, factors,
    small_sem, load_sem, state_sem, send_sem, x_sem, z_sem, a_sem, t_sem,
    st0_send, st0_recv, st1_send, st1_recv, end_in, core_in, y_in, middle_in, all_in,
):
    layers, rows = out.shape[0], out.shape[1]
    pieces = snd.shape[1]
    depth = snd.shape[2]
    per_layer = pieces // layers
    small = [
        pltpu.make_async_copy(src, dst, small_sem.at[i])
        for i, (src, dst) in enumerate(((mask_in, mask), (losses_in, losses), (weights_in, weights)))
    ]
    for copy in small:
        copy.start()

    dp, mp = lax.axis_index("dp"), lax.axis_index("mp")
    z, x = dp // 2, lax.rem(dp, 2)
    upper = z // 2
    place = lax.rem(z + upper, 2)

    def by_half(pair):
        return pair[0] + upper * (pair[1] - pair[0])

    early, start, paced_pieces = by_half(EARLY), by_half(START), by_half(PACED)
    tail = early - TAIL
    x_dev = z * 2 + 1 - x
    z_dev = (z + 1 - 2 * lax.rem(z, 2)) * 2 + x
    a_dev = (3 - z) * 2 + x

    barrier = pltpu.get_barrier_semaphore()
    devices = 8 * n_mp
    place_in_all = dp * n_mp + mp

    def away(i):
        other_z, other_x, other_mp = z ^ (i // (2 * n_mp)), x ^ (i // n_mp % 2), mp ^ (i % n_mp)
        other_dp = other_z * 2 + other_x
        return other_dp * n_mp + other_mp, {"dp": other_dp, "mp": other_mp}

    def greet(sem, device):
        pl.semaphore_signal(sem, inc=1, device_id=device, device_id_type=MESH_ID)

    def load(slot, layer):
        k, side = slot // 2, slot % 2
        target = (k + upper * (3 - 2 * k)) * 2 + x + side * (1 - 2 * x)
        return pltpu.make_async_copy(
            grads.at[0, layer, pl.ds(target * rows, rows), :], held.at[slot, layer], load_sem.at[slot, layer]
        )

    def fetch(*slots):
        for slot in slots:
            for layer in range(layers):
                load(slot, layer).start()

    def state():
        pairs = ((params_in, params_out), (moment_in, moment_out), (second_in, second_out))
        return [pltpu.make_async_copy(src, dst, state_sem.at[i]) for i, (src, dst) in enumerate(pairs)]

    raw = 3 - 2 * place
    load(7, 0).start()
    load(raw, 0).start()
    for device in ({"dp": x_dev}, {"dp": z_dev}):
        greet(barrier, device)

    @pl.when(place == 1)
    def _():
        for device in ({"dp": a_dev}, {"mp": mp ^ 1}, {"mp": mp ^ 2}):
            greet(barrier, device)

    load(7, 1).start()
    load(raw, 1).start()
    fetch(6, 5, 4 - raw, 4, 2, 0)

    def loaded(*slots):
        for slot in slots:
            for layer in range(layers):
                load(slot, layer).wait()

    for copy in small:
        copy.wait()
    lane = lax.broadcasted_iota(jnp.int32, st0.shape[1:], 1)
    tile = jnp.zeros(st0.shape[1:], jnp.float32)
    for layer in range(layers):
        keep = mask[0, layer].astype(jnp.float32)
        tile = jnp.where(lane == layer, keep, tile)
        tile = jnp.where(lane == layers + layer, keep * losses[0, layer], tile)
    st0[dp] = tile

    pl.when(place == 0)(lambda: pl.semaphore_wait(barrier, 2))
    pl.when(place == 1)(lambda: pl.semaphore_wait(barrier, 5))

    def meet():
        @pl.when(place == 0)
        def _():
            greet(end_in, {"dp": z_dev})
            pl.semaphore_wait(all_in, 1)

        @pl.when(place == 1)
        def _():
            pl.semaphore_wait(end_in, 1)
            greet(core_in, {"mp": mp ^ 1})
            pl.semaphore_wait(core_in, 1)
            greet(y_in, {"mp": mp ^ 2})
            pl.semaphore_wait(y_in, 1)
            greet(middle_in, {"dp": a_dev})
            pl.semaphore_wait(middle_in, 1)
            greet(all_in, {"dp": z_dev})

    def own(slot, c):
        layer, r = c // per_layer, lax.rem(c, per_layer)
        keep = mask[0, layer].astype(jnp.float32)
        return held[slot, layer, pl.ds(pl.multiple_of(r * depth, depth), depth), :].astype(jnp.float32) * keep

    def push(slot, c, dst, sem, device):
        return pltpu.make_async_remote_copy(
            src_ref=snd.at[slot, c], dst_ref=dst, send_sem=send_sem.at[slot], recv_sem=sem,
            device_id={"dp": device}, device_id_type=MESH_ID,
        )

    def to_x(k, c):
        return push(2 * k + OTHER, c, xr.at[k, c], x_sem.at[k, c], x_dev)

    def to_z(slot, box, c):
        return push(slot, c, zr.at[box, c], z_sem.at[box, c], z_dev)

    def to_a(k, c):
        return push(2 * k + MINE, c, ar.at[3 - k, c], a_sem.at[3 - k, c], a_dev)

    def to_tail(c):
        return push(2, c, tr.at[c - tail], t_sem.at[c - tail], z_dev)

    def from_tail(c):
        to_tail(c).wait_recv()
        return tr[c - tail]

    def from_x(k, c):
        to_x(k, c).wait_recv()
        return xr[k, c]

    def from_z(box, c):
        to_z(0, box, c).wait_recv()
        return zr[box, c]

    def from_a(box, c):
        to_a(3 - box, c).wait_recv()
        return ar[box, c]

    def each(low, high, step):
        def one(c, carry):
            step(c)
            return carry

        lax.fori_loop(low, high, one, 0)

    def x_own(k, c):
        snd[2 * k + OTHER, c] = own(2 * k + OTHER, c)
        to_x(k, c).start()

    def share_stats(i):
        return pltpu.make_async_remote_copy(
            src_ref=st0.at[dp], dst_ref=st0.at[dp], send_sem=st0_send.at[i], recv_sem=st0_recv.at[dp],
            device_id={"dp": lax.rem(dp + i, 8)}, device_id_type=MESH_ID,
        )

    def stats_arrival(i):
        peer = lax.rem(dp + i, 8)
        return pltpu.make_async_remote_copy(
            src_ref=st0.at[dp], dst_ref=st0.at[peer], send_sem=st0_send.at[i], recv_sem=st0_recv.at[peer],
            device_id={"dp": peer}, device_id_type=MESH_ID,
        )

    @pl.when(place == 0)
    def _():
        load(7, 0).wait()
        x_own(3, 0)
        load(3, 0).wait()

        def z_raw(c):
            snd[3, c] = own(3, c)
            to_z(3, 0, c).start()

        def first(c):
            x_own(3, c)
            pl.when(c < early)(lambda: z_raw(c))

        z_raw(0)
        each(1, per_layer, first)
        load(7, 1).wait()
        load(3, 1).wait()
        each(per_layer, pieces, first)
        meet()
        for copy in state():
            copy.start()
        loaded(1, 6, 5)
        for i in range(1, 8):
            share_stats(i).start()

        def second(c):
            snd[6, c] = own(6, c) + from_x(3, c)
            to_z(6, 3, c).start()
            x_own(2, c)

        each(0, pieces, second)
        loaded(4, 2, 0)

        def send_own_level(c):
            snd[1, c] = own(1, c) + from_z(1, c)
            to_x(0, c).start()

        def third(c):
            snd[4, c] = own(4, c) + from_x(2, c)
            to_z(4, 2, c).start()

        def third_a(c):
            third(c)
            x_own(1, c + early)

        def third_b(c):
            third(c)
            send_own_level(c - (pieces - early))

        each(0, pieces - early, third_a)
        each(pieces - early, pieces, third_b)

        def fourth(c):
            snd[2, c] = own(2, c) + from_x(1, c)
            to_z(2, 1, c).start()
            send_own_level(c)

        each(early, pieces, fourth)

        def fifth(c):
            snd[2, c] = own(2, c)
            to_z(2, 1, c).start()

        each(0, tail, fifth)

    @pl.when(place == 1)
    def _():
        load(7, 0).wait()
        load(1, 0).wait()

        def first(c):
            x_own(3, c)
            snd[1, c] = own(1, c)
            to_z(1, 1, c).start()

        each(0, per_layer, first)
        load(7, 1).wait()
        load(1, 1).wait()
        each(per_layer, pieces, first)
        meet()
        for copy in state():
            copy.start()
        loaded(3, 6, 5)
        for i in range(1, 8):
            share_stats(i).start()
        loaded(4, 2, 0)

        def pass_out(c):
            snd[0, c] = own(0, c) + from_a(0, c)
            to_z(0, 0, c).start()

        def second(c):
            x_own(2, c)

            @pl.when(c < early)
            def _():
                snd[3, c] = own(3, c) + from_z(0, c)
                to_x(1, c).start()

            snd[6, c] = own(6, c) + from_x(3, c) + from_z(3, c)
            to_a(3, c).start()

        def second_b(c):
            second(c)
            pass_out(c - LAG)

        each(0, LAG, second)
        each(LAG, pieces, second_b)

        def third(c):
            @pl.when(c < pieces - early)
            def _():
                x_own(1, c + early)

            snd[4, c] = own(4, c) + from_x(2, c) + from_z(2, c)
            to_a(2, c).start()

            @pl.when(c < LAG)
            def _():
                pass_out(c + pieces - LAG)

        def return_tail(c):
            snd[2, c] = own(2, c) + from_x(1, c) + from_a(1, c)
            to_tail(c).start()

        def third_b(c):
            third(c)
            return_tail(c - LAG)

        each(0, tail + LAG, third)
        each(tail + LAG, early + LAG, third_b)
        each(early + LAG, pieces, third)

    for copy in state():
        copy.wait()

    def weigh(ref, layer, c, factor):
        window = (layer, pl.ds(pl.multiple_of(c * depth, depth), depth))
        ref[window] = ref[window] * factor

    for layer in range(layers):
        def weigh_all(c, layer=layer):
            weigh(params_out, layer, c, 1.0 - learn_rate * decay_rate)
            weigh(moment_out, layer, c, beta_one)
            weigh(second_out, layer, c, beta_two)

        each(0, per_layer, weigh_all)

    for i in range(1, 8):
        stats_arrival(i).wait_recv()
    total = st0[0]
    for i in range(1, 8):
        total = total + st0[i]
    stats_out[...] = total
    weight_sum = weights[0].astype(jnp.float32)
    for layer in range(1, layers):
        weight_sum = weight_sum + weights[layer].astype(jnp.float32)
    square[...] = jnp.zeros_like(square)
    for layer in range(layers):
        factor = weights[layer].astype(jnp.float32) / (weight_sum * total[:, layer : layer + 1])
        factors[layer] = jnp.broadcast_to(factor, factors.shape[1:])

    def count(gradient):
        squares = gradient * gradient
        square[...] += jnp.sum(squares.reshape(depth // 8, 8, squares.shape[1]), axis=0)

    def finish(c, summed):
        layer, r = c // per_layer, lax.rem(c, per_layer)
        gradient = summed * factors[layer]
        out[layer, pl.ds(pl.multiple_of(r * depth, depth), depth), :] = gradient
        return gradient

    def last(c):
        count(finish(c, own(2, c) + from_x(1, c) + from_a(1, c) + from_z(1, c)))

    def finish_tail(c):
        finish(c, snd[2, c] + from_z(1, c))

    def last_end(c):
        count(finish(c, own(0, c) + from_z(0, c) + from_x(0, c)))

    def count_tail(c):
        snd[2, c] = own(2, c)
        count((snd[2, c] + from_tail(c)) * factors[c // per_layer])

    def paced(c):
        to_z(2, 1, c - start + tail).start()
        last_end(c)

    @pl.when(place == 0)
    def _():
        each(tail, early, count_tail)
        each(0, start, last_end)
        each(start, start + paced_pieces, paced)
        each(start + paced_pieces, pieces, last_end)

    @pl.when(place == 1)
    def _():
        each(early, pieces, last)
        each(0, tail, last)

    def share_square(i):
        return pltpu.make_async_remote_copy(
            src_ref=st1.at[place_in_all], dst_ref=st1.at[place_in_all],
            send_sem=st1_send.at[i], recv_sem=st1_recv.at[place_in_all],
            device_id=away(i)[1], device_id_type=MESH_ID,
        )

    def square_arrival(i):
        peer, device = away(i)
        return pltpu.make_async_remote_copy(
            src_ref=st1.at[place_in_all], dst_ref=st1.at[peer], send_sem=st1_send.at[i], recv_sem=st1_recv.at[peer],
            device_id=device, device_id_type=MESH_ID,
        )

    folded = jnp.sum(square[...], axis=0, keepdims=True)
    st1[place_in_all] = sum(folded[:, i : i + LANES] for i in range(0, folded.shape[1], LANES))
    for i in range(devices - 1, 0, -1):
        share_square(i).start()

    @pl.when(place == 0)
    def _():
        each(tail + paced_pieces, early, lambda c: to_z(2, 1, c).start())

    @pl.when(place == 1)
    def _():
        each(tail, early, finish_tail)

    for i in range(1, 8):
        share_stats(i).wait_send()
    for i in range(1, devices):
        share_square(i).wait_send()

    def sent(slot, size=pieces):
        pltpu.make_async_remote_copy(
            src_ref=snd.at[slot, pl.ds(0, size)], dst_ref=zr.at[0, pl.ds(0, size)],
            send_sem=send_sem.at[slot], recv_sem=z_sem.at[0, 0],
            device_id={"dp": z_dev}, device_id_type=MESH_ID,
        ).wait_send()

    for slot in (1, 3, 4, 5, 6, 7):
        sent(slot)

    @pl.when(place == 0)
    def _():
        sent(2)

    @pl.when(place == 1)
    def _():
        sent(0)
        sent(2, TAIL)

    for i in range(1, devices):
        square_arrival(i).wait_recv()
    square_sum = jnp.sum(jnp.sum(st1[...], axis=0), keepdims=True)
    rms_value = jnp.sqrt(square_sum / entries)
    clip_out[...] = jnp.broadcast_to(jnp.minimum(1.0, max_rms / (rms_value + eps_norm)), clip_out.shape)


def update_kernel(gradient, params, moment, second, stats, clip, params_out, moment_out, second_out, mean_out, news, mean, sem, mean_sem):
    layers, rows = gradient.shape[0], gradient.shape[1]
    outs = (params_out, moment_out, second_out)
    chunk, step = min(CHUNK, rows), min(STEP, rows)
    mean[...] = stats[:, layers : 2 * layers] / stats[:, :layers]
    mean_copy = pltpu.make_async_copy(mean, mean_out, mean_sem)
    mean_copy.start()
    clip_scale = clip[...]
    first_scale = (1.0 - beta_one) * clip_scale
    second_scale = (1.0 - beta_two) * clip_scale * clip_scale

    def put(i, layer, low):
        window = (layer, pl.ds(low, chunk))
        return pltpu.make_async_copy(news.at[(i, *window)], outs[i].at[window], sem.at[i])

    chunks = [(layer, low) for layer in range(layers) for low in range(0, rows, chunk)]
    for layer, low in chunks:
        for start in range(low, low + chunk, step):
            window = (layer, pl.ds(start, step))
            held = gradient[window]
            new_moment = moment[window] + first_scale * held
            new_second = second[window] + second_scale * (held * held)
            root = new_second * lax.rsqrt(new_second)
            news[(0, *window)] = params[window] - learn_rate * (new_moment / (root + eps_adam))
            news[(1, *window)] = new_moment
            news[(2, *window)] = new_second
        for i in range(3):
            put(i, layer, low).start()
    for i in range(3):
        pltpu.make_async_copy(news.at[i], outs[i], sem.at[i]).wait()
    mean_copy.wait()


def line_body(n_mp, entries, gradients, layer_mask, exit_losses, exit_weights, params, moment, second):
    layers, rows, columns = params.shape
    depth = min(ROWS, rows)
    pieces = layers * (rows // depth)
    vmem, hbm = pl.BlockSpec(memory_space=pltpu.VMEM), pl.BlockSpec(memory_space=pltpu.HBM)
    block = (pieces, depth, columns)
    f32, dma, regular = jnp.float32, pltpu.SemaphoreType.DMA, pltpu.SemaphoreType.REGULAR
    state = jax.ShapeDtypeStruct((layers, rows, columns), f32)

    def kernel(*refs):
        pl.run_scoped(lambda *sems: line_kernel(n_mp, entries, *refs, *sems),
            dma((3,)), dma((8, layers)), dma((3,)), dma((8,)), dma((4, pieces)), dma((4, pieces)), dma((2, pieces)), dma((TAIL,)),
            dma((8,)), dma((8,)), dma((8 * n_mp,)), dma((8 * n_mp,)), regular, regular, regular, regular, regular,
        )

    *held, stats, clip = pl.pallas_call(
        kernel,
        name="line_reduce",
        out_shape=(
            state, state, state, state,
            jax.ShapeDtypeStruct((1, LANES), f32),
            jax.ShapeDtypeStruct((1, columns), f32),
        ),
        in_specs=[hbm] * 7,
        out_specs=[vmem] * 6,
        scratch_shapes=[
            pltpu.SMEM(layer_mask.shape, layer_mask.dtype),
            pltpu.SMEM(exit_losses.shape, exit_losses.dtype),
            pltpu.SMEM(exit_weights.shape, exit_weights.dtype),
            pltpu.VMEM((8, layers, rows, columns), gradients.dtype),
            pltpu.VMEM((8, *block), f32),
            pltpu.VMEM((4, *block), f32),
            pltpu.VMEM((4, *block), f32),
            pltpu.VMEM((2, *block), f32),
            pltpu.VMEM((TAIL, *block[1:]), f32),
            pltpu.VMEM((8, 1, LANES), f32),
            pltpu.VMEM((8 * n_mp, 1, LANES), f32),
            pltpu.VMEM((8, columns), f32),
            pltpu.VMEM((layers, 1, columns), f32),
        ],
        compiler_params=pltpu.CompilerParams(
            collective_id=0, has_side_effects=True, vmem_limit_bytes=40 * 1024 * 1024
        ),
    )(*(
        pltpu.with_memory_space_constraint(a, pltpu.HBM)
        for a in (layer_mask, exit_losses, exit_weights, gradients, params, moment, second)
    ))
    *new, mean = pl.pallas_call(
        update_kernel,
        name="update",
        out_shape=(state, state, state, jax.ShapeDtypeStruct((1, layers), f32)),
        in_specs=[vmem] * 6,
        out_specs=[hbm] * 4,
        scratch_shapes=[pltpu.VMEM((3, layers, rows, columns), f32), pltpu.VMEM((1, layers), f32), dma((3,)), dma],
        compiler_params=pltpu.CompilerParams(vmem_limit_bytes=16 * 1024 * 1024),
    )(*held, stats, clip)
    return (*new, mean[0])


def solution(mesh):
    state = P(None, "dp", "mp")
    placed = (P("dp", None, None, "mp"), P("dp", None), P("dp", None), P(), state, state, state)
    n_dp, n_mp = mesh.shape["dp"], mesh.shape["mp"]

    def whole(*args):
        entries = args[4].size
        layers = args[4].shape[0]

        def body(*blocks):
            if n_dp == 8 and n_mp == 4 and layers == 2:
                return line_body(n_mp, entries, *blocks)
            return any_mesh_body(entries, *blocks)

        return jax.shard_map(
            body, mesh=mesh, in_specs=placed, out_specs=(state, state, state, P()), check_vma=False
        )(*args)

    return whole
```

```python
import jax
import jax.numpy as jnp
from jax import lax
from jax.experimental import pallas as pl
from jax.experimental.pallas import tpu as pltpu
from jax.sharding import PartitionSpec as P

max_rms = 1.0
eps_norm = 1e-06
eps_adam = 1e-08
beta_one = 0.9
beta_two = 0.95
learn_rate = 0.01
decay_rate = 0.1

MESH_ID = pl.DeviceIdType.MESH
ROWS = 32
LANES = 128
LAG = 8
EARLY = (18, 21)
START = (19, 25)
PACED = (10, 4)
TAIL = 12
HEAD = 2
CHUNK = 64
STEP = 16
MINE, OTHER = 0, 1


def update(gradient, clip_scale, params, moment, second):
    clipped = clip_scale * gradient
    new_moment = beta_one * moment + (1.0 - beta_one) * clipped
    new_second = beta_two * second + (1.0 - beta_two) * clipped * clipped
    new_params = params - learn_rate * (
        new_moment / (jnp.sqrt(new_second) + eps_adam) + decay_rate * params
    )
    return new_params, new_moment, new_second


def any_mesh_body(entries, gradients, layer_mask, exit_losses, exit_weights, params, moment, second):
    keep_float = layer_mask[0].astype(jnp.float32)
    loss_terms = keep_float * exit_losses[0]
    local_term = gradients[0].astype(jnp.float32) * keep_float[:, None, None]
    summed = lax.psum_scatter(local_term, "dp", scatter_dimension=1, tiled=True)
    weight_float = exit_weights.astype(jnp.float32)
    weight_sum = jnp.sum(weight_float)
    layer_count, loss_sum = lax.psum((keep_float, loss_terms), "dp")
    gradient = summed * (weight_float / (weight_sum * layer_count))[:, None, None]
    square_sum = lax.psum(jnp.sum(gradient * gradient), ("dp", "mp"))
    rms_value = jnp.sqrt(square_sum / entries)
    clip_scale = jnp.minimum(1.0, max_rms / (rms_value + eps_norm))
    new = update(gradient, clip_scale, params, moment, second)
    return (*new, loss_sum / layer_count)


def line_kernel(
    n_mp, entries, mask_in, losses_in, weights_in, grads, params_in, moment_in, second_in,
    out, params_out, moment_out, second_out, stats_out, clip_out,
    mask, losses, weights, held, snd, xr, zr, ar, tr, st0, st1, square, factors,
    small_sem, head_sem, load_sem, state_sem, send_sem, x_sem, z_sem, a_sem, t_sem,
    st0_send, st0_recv, st1_send, st1_recv, end_in, core_in, y_in, middle_in, all_in,
):
    layers, rows = out.shape[0], out.shape[1]
    pieces = snd.shape[1]
    depth = snd.shape[2]
    per_layer = pieces // layers
    dp, mp = lax.axis_index("dp"), lax.axis_index("mp")
    z, x = dp // 2, lax.rem(dp, 2)
    upper = z // 2
    place = lax.rem(z + upper, 2)

    def by_half(pair):
        return pair[0] + upper * (pair[1] - pair[0])

    early, start, paced_pieces = by_half(EARLY), by_half(START), by_half(PACED)
    tail = early - TAIL
    x_dev = z * 2 + 1 - x
    z_dev = (z + 1 - 2 * lax.rem(z, 2)) * 2 + x
    a_dev = (3 - z) * 2 + x

    barrier = pltpu.get_barrier_semaphore()
    devices = 8 * n_mp
    place_in_all = dp * n_mp + mp

    def away(i):
        other_z, other_x, other_mp = z ^ (i // (2 * n_mp)), x ^ (i // n_mp % 2), mp ^ (i % n_mp)
        other_dp = other_z * 2 + other_x
        return other_dp * n_mp + other_mp, {"dp": other_dp, "mp": other_mp}

    def greet(sem, device):
        pl.semaphore_signal(sem, inc=1, device_id=device, device_id_type=MESH_ID)

    greet(barrier, {"dp": x_dev})

    def load(slot, layer, low=0, high=rows, sem=None):
        k, side = slot // 2, slot % 2
        target = (k + upper * (3 - 2 * k)) * 2 + x + side * (1 - 2 * x)
        return pltpu.make_async_copy(
            grads.at[0, layer, pl.ds(target * rows + low, high - low), :],
            held.at[slot, layer, pl.ds(low, high - low)],
            load_sem.at[slot, layer] if sem is None else head_sem.at[sem],
        )

    def load_head(i):
        return load((7, raw)[i], 0, 0, HEAD * depth, i)

    def load_body(i):
        return load((7, raw)[i], 0, HEAD * depth)

    raw = 3 - 2 * place
    small = [
        pltpu.make_async_copy(src, dst, small_sem.at[i])
        for i, (src, dst) in enumerate(((mask_in, mask), (losses_in, losses), (weights_in, weights)))
    ]
    small[0].start()
    load_head(0).start()
    load_head(1).start()
    greet(barrier, {"dp": z_dev})

    @pl.when(place == 1)
    def _():
        for device in ({"dp": a_dev}, {"mp": mp ^ 1}, {"mp": mp ^ 2}):
            greet(barrier, device)

    load_body(0).start()
    load_body(1).start()

    def fetch(*slots):
        for slot in slots:
            for layer in range(layers):
                load(slot, layer).start()

    def state():
        pairs = ((params_in, params_out), (moment_in, moment_out), (second_in, second_out))
        return [pltpu.make_async_copy(src, dst, state_sem.at[i]) for i, (src, dst) in enumerate(pairs)]

    load(7, 1).start()
    load(raw, 1).start()
    fetch(6, 5, 4 - raw, 4, 2, 0)
    for copy in small[1:]:
        copy.start()

    def loaded(*slots):
        for slot in slots:
            for layer in range(layers):
                load(slot, layer).wait()

    small[0].wait()
    pl.when(place == 0)(lambda: pl.semaphore_wait(barrier, 2))
    pl.when(place == 1)(lambda: pl.semaphore_wait(barrier, 5))

    def set_stats():
        for copy in small[1:]:
            copy.wait()
        lane = lax.broadcasted_iota(jnp.int32, st0.shape[1:], 1)
        tile = jnp.zeros(st0.shape[1:], jnp.float32)
        for layer in range(layers):
            keep = mask[0, layer].astype(jnp.float32)
            tile = jnp.where(lane == layer, keep, tile)
            tile = jnp.where(lane == layers + layer, keep * losses[0, layer], tile)
        st0[dp] = tile

    def meet():
        @pl.when(place == 0)
        def _():
            greet(end_in, {"dp": z_dev})
            pl.semaphore_wait(all_in, 1)

        @pl.when(place == 1)
        def _():
            pl.semaphore_wait(end_in, 1)
            greet(core_in, {"mp": mp ^ 1})
            pl.semaphore_wait(core_in, 1)
            greet(y_in, {"mp": mp ^ 2})
            pl.semaphore_wait(y_in, 1)
            greet(middle_in, {"dp": a_dev})
            pl.semaphore_wait(middle_in, 1)
            greet(all_in, {"dp": z_dev})

    def own(slot, c):
        layer, r = c // per_layer, lax.rem(c, per_layer)
        keep = mask[0, layer].astype(jnp.float32)
        return held[slot, layer, pl.ds(pl.multiple_of(r * depth, depth), depth), :].astype(jnp.float32) * keep

    def push(slot, c, dst, sem, device):
        return pltpu.make_async_remote_copy(
            src_ref=snd.at[slot, c], dst_ref=dst, send_sem=send_sem.at[slot], recv_sem=sem,
            device_id={"dp": device}, device_id_type=MESH_ID,
        )

    def to_x(k, c):
        return push(2 * k + OTHER, c, xr.at[k, c], x_sem.at[k, c], x_dev)

    def to_z(slot, box, c):
        return push(slot, c, zr.at[box, c], z_sem.at[box, c], z_dev)

    def to_a(k, c):
        return push(2 * k + MINE, c, ar.at[3 - k, c], a_sem.at[3 - k, c], a_dev)

    def to_tail(c):
        return push(2, c, tr.at[c - tail], t_sem.at[c - tail], z_dev)

    def from_tail(c):
        to_tail(c).wait_recv()
        return tr[c - tail]

    def from_x(k, c):
        to_x(k, c).wait_recv()
        return xr[k, c]

    def from_z(box, c):
        to_z(0, box, c).wait_recv()
        return zr[box, c]

    def from_a(box, c):
        to_a(3 - box, c).wait_recv()
        return ar[box, c]

    def each(low, high, step):
        def one(c, carry):
            step(c)
            return carry

        lax.fori_loop(low, high, one, 0)

    def x_own(k, c):
        snd[2 * k + OTHER, c] = own(2 * k + OTHER, c)
        to_x(k, c).start()

    def share_stats(i):
        return pltpu.make_async_remote_copy(
            src_ref=st0.at[dp], dst_ref=st0.at[dp], send_sem=st0_send.at[i], recv_sem=st0_recv.at[dp],
            device_id={"dp": lax.rem(dp + i, 8)}, device_id_type=MESH_ID,
        )

    def stats_arrival(i):
        peer = lax.rem(dp + i, 8)
        return pltpu.make_async_remote_copy(
            src_ref=st0.at[dp], dst_ref=st0.at[peer], send_sem=st0_send.at[i], recv_sem=st0_recv.at[peer],
            device_id={"dp": peer}, device_id_type=MESH_ID,
        )

    @pl.when(place == 0)
    def _():
        def z_raw(c):
            snd[3, c] = own(3, c)
            to_z(3, 0, c).start()

        def first(c):
            x_own(3, c)
            pl.when(c < early)(lambda: z_raw(c))

        load_head(0).wait()
        x_own(3, 0)
        load_head(1).wait()
        z_raw(0)
        each(1, HEAD, first)
        load_body(0).wait()
        load_body(1).wait()
        each(HEAD, per_layer, first)
        load(7, 1).wait()
        load(3, 1).wait()
        each(per_layer, pieces, first)
        meet()
        for copy in state():
            copy.start()
        loaded(1, 6, 5)
        set_stats()
        for i in range(1, 8):
            share_stats(i).start()

        def second(c):
            snd[6, c] = own(6, c) + from_x(3, c)
            to_z(6, 3, c).start()
            x_own(2, c)

        each(0, pieces, second)
        loaded(4, 2, 0)

        def send_own_level(c):
            snd[1, c] = own(1, c) + from_z(1, c)
            to_x(0, c).start()

        def third(c):
            snd[4, c] = own(4, c) + from_x(2, c)
            to_z(4, 2, c).start()

        def third_a(c):
            third(c)
            x_own(1, c + early)

        def third_b(c):
            third(c)
            send_own_level(c - (pieces - early))

        each(0, pieces - early, third_a)
        each(pieces - early, pieces, third_b)

        def fourth(c):
            snd[2, c] = own(2, c) + from_x(1, c)
            to_z(2, 1, c).start()
            send_own_level(c)

        each(early, pieces, fourth)

        def fifth(c):
            snd[2, c] = own(2, c)
            to_z(2, 1, c).start()

        each(0, tail, fifth)

    @pl.when(place == 1)
    def _():
        load_head(0).wait()
        load_head(1).wait()

        def first(c):
            x_own(3, c)
            snd[1, c] = own(1, c)
            to_z(1, 1, c).start()

        each(0, HEAD, first)
        load_body(0).wait()
        load_body(1).wait()
        each(HEAD, per_layer, first)
        load(7, 1).wait()
        load(1, 1).wait()
        each(per_layer, pieces, first)
        meet()
        for copy in state():
            copy.start()
        loaded(3, 6, 5)
        set_stats()
        for i in range(1, 8):
            share_stats(i).start()
        loaded(4, 2, 0)

        def pass_out(c):
            snd[0, c] = own(0, c) + from_a(0, c)
            to_z(0, 0, c).start()

        def second(c):
            x_own(2, c)

            @pl.when(c < early)
            def _():
                snd[3, c] = own(3, c) + from_z(0, c)
                to_x(1, c).start()

            snd[6, c] = own(6, c) + from_x(3, c) + from_z(3, c)
            to_a(3, c).start()

        def second_b(c):
            second(c)
            pass_out(c - LAG)

        each(0, LAG, second)
        each(LAG, pieces, second_b)

        def third(c):
            @pl.when(c < pieces - early)
            def _():
                x_own(1, c + early)

            snd[4, c] = own(4, c) + from_x(2, c) + from_z(2, c)
            to_a(2, c).start()

            @pl.when(c < LAG)
            def _():
                pass_out(c + pieces - LAG)

        def return_tail(c):
            snd[2, c] = own(2, c) + from_x(1, c) + from_a(1, c)
            to_tail(c).start()

        def third_b(c):
            third(c)
            return_tail(c - LAG)

        each(0, tail + LAG, third)
        each(tail + LAG, early + LAG, third_b)
        each(early + LAG, pieces, third)

    for copy in state():
        copy.wait()

    def weigh(ref, layer, c, factor):
        window = (layer, pl.ds(pl.multiple_of(c * depth, depth), depth))
        ref[window] = ref[window] * factor

    for layer in range(layers):
        def weigh_all(c, layer=layer):
            weigh(params_out, layer, c, 1.0 - learn_rate * decay_rate)
            weigh(moment_out, layer, c, beta_one)
            weigh(second_out, layer, c, beta_two)

        each(0, per_layer, weigh_all)

    for i in range(1, 8):
        stats_arrival(i).wait_recv()
    total = st0[0]
    for i in range(1, 8):
        total = total + st0[i]
    stats_out[...] = total
    weight_sum = weights[0].astype(jnp.float32)
    for layer in range(1, layers):
        weight_sum = weight_sum + weights[layer].astype(jnp.float32)
    square[...] = jnp.zeros_like(square)
    for layer in range(layers):
        factor = weights[layer].astype(jnp.float32) / (weight_sum * total[:, layer : layer + 1])
        factors[layer] = jnp.broadcast_to(factor, factors.shape[1:])

    def count(gradient):
        squares = gradient * gradient
        square[...] += jnp.sum(squares.reshape(depth // 8, 8, squares.shape[1]), axis=0)

    def finish(c, summed):
        layer, r = c // per_layer, lax.rem(c, per_layer)
        gradient = summed * factors[layer]
        out[layer, pl.ds(pl.multiple_of(r * depth, depth), depth), :] = gradient
        return gradient

    def last(c):
        count(finish(c, own(2, c) + from_x(1, c) + from_a(1, c) + from_z(1, c)))

    def finish_tail(c):
        finish(c, snd[2, c] + from_z(1, c))

    def last_end(c):
        count(finish(c, own(0, c) + from_z(0, c) + from_x(0, c)))

    def count_tail(c):
        snd[2, c] = own(2, c)
        count((snd[2, c] + from_tail(c)) * factors[c // per_layer])

    def paced(c):
        to_z(2, 1, c - start + tail).start()
        last_end(c)

    @pl.when(place == 0)
    def _():
        each(tail, early, count_tail)
        each(0, start, last_end)
        each(start, start + paced_pieces, paced)
        each(start + paced_pieces, pieces, last_end)

    @pl.when(place == 1)
    def _():
        each(early, pieces, last)
        each(0, tail, last)

    def share_square(i):
        return pltpu.make_async_remote_copy(
            src_ref=st1.at[place_in_all], dst_ref=st1.at[place_in_all],
            send_sem=st1_send.at[i], recv_sem=st1_recv.at[place_in_all],
            device_id=away(i)[1], device_id_type=MESH_ID,
        )

    def square_arrival(i):
        peer, device = away(i)
        return pltpu.make_async_remote_copy(
            src_ref=st1.at[place_in_all], dst_ref=st1.at[peer], send_sem=st1_send.at[i], recv_sem=st1_recv.at[peer],
            device_id=device, device_id_type=MESH_ID,
        )

    folded = jnp.sum(square[...], axis=0, keepdims=True)
    st1[place_in_all] = sum(folded[:, i : i + LANES] for i in range(0, folded.shape[1], LANES))
    for i in range(devices - 1, 0, -1):
        share_square(i).start()

    @pl.when(place == 0)
    def _():
        each(tail + paced_pieces, early, lambda c: to_z(2, 1, c).start())

    for i in range(1, 8):
        share_stats(i).wait_send()
    for i in range(1, devices):
        share_square(i).wait_send()

    def sent(slot, size=pieces):
        pltpu.make_async_remote_copy(
            src_ref=snd.at[slot, pl.ds(0, size)], dst_ref=zr.at[0, pl.ds(0, size)],
            send_sem=send_sem.at[slot], recv_sem=z_sem.at[0, 0],
            device_id={"dp": z_dev}, device_id_type=MESH_ID,
        ).wait_send()

    for slot in (1, 3, 4, 5, 6, 7):
        sent(slot)

    @pl.when(place == 0)
    def _():
        sent(2)

    @pl.when(place == 1)
    def _():
        sent(0)
        sent(2, TAIL)

    for i in range(1, devices):
        square_arrival(i).wait_recv()
    square_sum = jnp.sum(jnp.sum(st1[...], axis=0), keepdims=True)
    rms_value = jnp.sqrt(square_sum / entries)
    clip_out[...] = jnp.broadcast_to(jnp.minimum(1.0, max_rms / (rms_value + eps_norm)), clip_out.shape)

    @pl.when(place == 1)
    def _():
        each(tail, early, finish_tail)


def update_kernel(gradient, params, moment, second, stats, clip, params_out, moment_out, second_out, mean_out, news, mean, sem, mean_sem):
    layers, rows = gradient.shape[0], gradient.shape[1]
    outs = (params_out, moment_out, second_out)
    chunk, step = min(CHUNK, rows), min(STEP, rows)
    mean[...] = stats[:, layers : 2 * layers] / stats[:, :layers]
    mean_copy = pltpu.make_async_copy(mean, mean_out, mean_sem)
    mean_copy.start()
    clip_scale = clip[...]
    first_scale = (1.0 - beta_one) * clip_scale
    second_scale = (1.0 - beta_two) * clip_scale * clip_scale

    def put(i, layer, low):
        window = (layer, pl.ds(low, chunk))
        return pltpu.make_async_copy(news.at[(i, *window)], outs[i].at[window], sem.at[i])

    chunks = [(layer, low) for layer in range(layers) for low in range(0, rows, chunk)]
    for layer, low in chunks:
        for start in range(low, low + chunk, step):
            window = (layer, pl.ds(start, step))
            held = gradient[window]
            new_moment = moment[window] + first_scale * held
            new_second = second[window] + second_scale * (held * held)
            root = new_second * lax.rsqrt(new_second)
            news[(0, *window)] = params[window] - learn_rate * (new_moment / (root + eps_adam))
            news[(1, *window)] = new_moment
            news[(2, *window)] = new_second
        for i in range(3):
            put(i, layer, low).start()
    for i in range(3):
        pltpu.make_async_copy(news.at[i], outs[i], sem.at[i]).wait()
    mean_copy.wait()


def line_body(n_mp, entries, gradients, layer_mask, exit_losses, exit_weights, params, moment, second):
    layers, rows, columns = params.shape
    depth = min(ROWS, rows)
    pieces = layers * (rows // depth)
    vmem, hbm = pl.BlockSpec(memory_space=pltpu.VMEM), pl.BlockSpec(memory_space=pltpu.HBM)
    block = (pieces, depth, columns)
    f32, dma, regular = jnp.float32, pltpu.SemaphoreType.DMA, pltpu.SemaphoreType.REGULAR
    state = jax.ShapeDtypeStruct((layers, rows, columns), f32)

    def kernel(*refs):
        pl.run_scoped(lambda *sems: line_kernel(n_mp, entries, *refs, *sems),
            dma((3,)), dma((2,)), dma((8, layers)), dma((3,)), dma((8,)), dma((4, pieces)), dma((4, pieces)), dma((2, pieces)), dma((TAIL,)),
            dma((8,)), dma((8,)), dma((8 * n_mp,)), dma((8 * n_mp,)), regular, regular, regular, regular, regular,
        )

    *held, stats, clip = pl.pallas_call(
        kernel,
        name="line_reduce",
        out_shape=(
            state, state, state, state,
            jax.ShapeDtypeStruct((1, LANES), f32),
            jax.ShapeDtypeStruct((1, columns), f32),
        ),
        in_specs=[hbm] * 7,
        out_specs=[vmem] * 6,
        scratch_shapes=[
            pltpu.SMEM(layer_mask.shape, layer_mask.dtype),
            pltpu.SMEM(exit_losses.shape, exit_losses.dtype),
            pltpu.SMEM(exit_weights.shape, exit_weights.dtype),
            pltpu.VMEM((8, layers, rows, columns), gradients.dtype),
            pltpu.VMEM((8, *block), f32),
            pltpu.VMEM((4, *block), f32),
            pltpu.VMEM((4, *block), f32),
            pltpu.VMEM((2, *block), f32),
            pltpu.VMEM((TAIL, *block[1:]), f32),
            pltpu.VMEM((8, 1, LANES), f32),
            pltpu.VMEM((8 * n_mp, 1, LANES), f32),
            pltpu.VMEM((8, columns), f32),
            pltpu.VMEM((layers, 1, columns), f32),
        ],
        compiler_params=pltpu.CompilerParams(
            collective_id=0, has_side_effects=True, vmem_limit_bytes=40 * 1024 * 1024
        ),
    )(*(
        pltpu.with_memory_space_constraint(a, pltpu.HBM)
        for a in (layer_mask, exit_losses, exit_weights, gradients, params, moment, second)
    ))
    *new, mean = pl.pallas_call(
        update_kernel,
        name="update",
        out_shape=(state, state, state, jax.ShapeDtypeStruct((1, layers), f32)),
        in_specs=[vmem] * 6,
        out_specs=[hbm] * 4,
        scratch_shapes=[pltpu.VMEM((3, layers, rows, columns), f32), pltpu.VMEM((1, layers), f32), dma((3,)), dma],
        compiler_params=pltpu.CompilerParams(vmem_limit_bytes=16 * 1024 * 1024),
    )(*held, stats, clip)
    return (*new, mean[0])


def solution(mesh):
    state = P(None, "dp", "mp")
    placed = (P("dp", None, None, "mp"), P("dp", None), P("dp", None), P(), state, state, state)
    n_dp, n_mp = mesh.shape["dp"], mesh.shape["mp"]

    def whole(*args):
        entries = args[4].size
        layers = args[4].shape[0]

        def body(*blocks):
            if n_dp == 8 and n_mp == 4 and layers == 2:
                return line_body(n_mp, entries, *blocks)
            return any_mesh_body(entries, *blocks)

        return jax.shard_map(
            body, mesh=mesh, in_specs=placed, out_specs=(state, state, state, P()), check_vma=False
        )(*args)

    return whole
```

```python
import jax
import jax.numpy as jnp
from jax import lax
from jax.experimental import pallas as pl
from jax.experimental.pallas import tpu as pltpu
from jax.sharding import PartitionSpec as P

max_rms = 1.0
eps_norm = 1e-06
eps_adam = 1e-08
beta_one = 0.9
beta_two = 0.95
learn_rate = 0.01
decay_rate = 0.1

MESH_ID = pl.DeviceIdType.MESH
ROWS = 32
PIECES = 32
LANES = 128
LAG = 8
EARLY = (18, 21)
START = (18, 24)
PACED = (11, 5)
TAIL = 13
HEAD = 2
CHUNK = 64
STEP = 16
MINE, OTHER = 0, 1


def update(gradient, clip_scale, params, moment, second):
    clipped = clip_scale * gradient
    new_moment = beta_one * moment + (1.0 - beta_one) * clipped
    new_second = beta_two * second + (1.0 - beta_two) * clipped * clipped
    new_params = params - learn_rate * (
        new_moment / (jnp.sqrt(new_second) + eps_adam) + decay_rate * params
    )
    return new_params, new_moment, new_second


def any_mesh_body(entries, gradients, layer_mask, exit_losses, exit_weights, params, moment, second):
    keep_float = layer_mask[0].astype(jnp.float32)
    loss_terms = keep_float * exit_losses[0]
    local_term = gradients[0].astype(jnp.float32) * keep_float[:, None, None]
    summed = lax.psum_scatter(local_term, "dp", scatter_dimension=1, tiled=True)
    weight_float = exit_weights.astype(jnp.float32)
    weight_sum = jnp.sum(weight_float)
    layer_count, loss_sum = lax.psum((keep_float, loss_terms), "dp")
    gradient = summed * (weight_float / (weight_sum * layer_count))[:, None, None]
    square_sum = lax.psum(jnp.sum(gradient * gradient), ("dp", "mp"))
    rms_value = jnp.sqrt(square_sum / entries)
    clip_scale = jnp.minimum(1.0, max_rms / (rms_value + eps_norm))
    new = update(gradient, clip_scale, params, moment, second)
    return (*new, loss_sum / layer_count)


def line_kernel(
    n_mp, entries, mask_in, losses_in, weights_in, grads, params_in, moment_in, second_in,
    out, params_out, moment_out, second_out, stats_out, clip_out,
    mask, losses, weights, held, snd, xr, zr, ar, tr, st0, st1, square, factors,
    small_sem, head_sem, load_sem, state_sem, send_sem, x_sem, z_sem, a_sem, t_sem,
    st0_send, st0_recv, st1_send, st1_recv, end_in, core_in, y_in, middle_in, all_in,
):
    layers, rows = out.shape[0], out.shape[1]
    pieces = snd.shape[1]
    depth = snd.shape[2]
    per_layer = pieces // layers
    dp, mp = lax.axis_index("dp"), lax.axis_index("mp")
    z, x = dp // 2, lax.rem(dp, 2)
    upper = z // 2
    place = lax.rem(z + upper, 2)

    def by_half(pair):
        return pair[0] + upper * (pair[1] - pair[0])

    early, start, paced_pieces = by_half(EARLY), by_half(START), by_half(PACED)
    tail = early - TAIL
    x_dev = z * 2 + 1 - x
    z_dev = (z + 1 - 2 * lax.rem(z, 2)) * 2 + x
    a_dev = (3 - z) * 2 + x

    barrier = pltpu.get_barrier_semaphore()
    devices = 8 * n_mp
    place_in_all = dp * n_mp + mp

    def away(i):
        other_z, other_x, other_mp = z ^ (i // (2 * n_mp)), x ^ (i // n_mp % 2), mp ^ (i % n_mp)
        other_dp = other_z * 2 + other_x
        return other_dp * n_mp + other_mp, {"dp": other_dp, "mp": other_mp}

    def greet(sem, device):
        pl.semaphore_signal(sem, inc=1, device_id=device, device_id_type=MESH_ID)

    def load(slot, layer, low=0, high=rows, sem=None):
        k, side = slot // 2, slot % 2
        target = (k + upper * (3 - 2 * k)) * 2 + x + side * (1 - 2 * x)
        return pltpu.make_async_copy(
            grads.at[0, layer, pl.ds(target * rows + low, high - low), :],
            held.at[slot, layer, pl.ds(low, high - low)],
            load_sem.at[slot, layer] if sem is None else head_sem.at[sem],
        )

    def load_head(i):
        return load((7, raw)[i], 0, 0, HEAD * depth, i)

    def load_body(i):
        return load((7, raw)[i], 0, HEAD * depth)

    raw = 3 - 2 * place
    small = [
        pltpu.make_async_copy(src, dst, small_sem.at[i])
        for i, (src, dst) in enumerate(((mask_in, mask), (losses_in, losses), (weights_in, weights)))
    ]
    small[0].start()
    load_head(0).start()
    load_head(1).start()
    greet(barrier, {"dp": x_dev})
    greet(barrier, {"dp": z_dev})

    @pl.when(place == 1)
    def _():
        for device in ({"dp": a_dev}, {"mp": mp ^ 1}, {"mp": mp ^ 2}):
            greet(barrier, device)

    load_body(0).start()
    load_body(1).start()

    def fetch(*slots):
        for slot in slots:
            for layer in range(layers):
                load(slot, layer).start()

    def state():
        pairs = ((params_in, params_out), (moment_in, moment_out), (second_in, second_out))
        return [pltpu.make_async_copy(src, dst, state_sem.at[i]) for i, (src, dst) in enumerate(pairs)]

    load(7, 1).start()
    load(raw, 1).start()
    fetch(6, 5, 4 - raw, 4, 2, 0)
    for copy in small[1:]:
        copy.start()

    def loaded(*slots):
        for slot in slots:
            for layer in range(layers):
                load(slot, layer).wait()

    small[0].wait()
    pl.when(place == 0)(lambda: pl.semaphore_wait(barrier, 2))
    pl.when(place == 1)(lambda: pl.semaphore_wait(barrier, 5))

    def set_stats():
        for copy in small[1:]:
            copy.wait()
        lane = lax.broadcasted_iota(jnp.int32, st0.shape[1:], 1)
        tile = jnp.zeros(st0.shape[1:], jnp.float32)
        for layer in range(layers):
            keep = mask[0, layer].astype(jnp.float32)
            tile = jnp.where(lane == layer, keep, tile)
            tile = jnp.where(lane == layers + layer, keep * losses[0, layer], tile)
        st0[dp] = tile

    def meet():
        @pl.when(place == 0)
        def _():
            greet(end_in, {"dp": z_dev})
            pl.semaphore_wait(all_in, 1)

        @pl.when(place == 1)
        def _():
            pl.semaphore_wait(end_in, 1)
            greet(core_in, {"mp": mp ^ 1})
            pl.semaphore_wait(core_in, 1)
            greet(y_in, {"mp": mp ^ 2})
            pl.semaphore_wait(y_in, 1)
            greet(middle_in, {"dp": a_dev})
            pl.semaphore_wait(middle_in, 1)
            greet(all_in, {"dp": z_dev})

    def own(slot, c):
        layer, r = c // per_layer, lax.rem(c, per_layer)
        keep = mask[0, layer].astype(jnp.float32)
        return held[slot, layer, pl.ds(pl.multiple_of(r * depth, depth), depth), :].astype(jnp.float32) * keep

    def push(slot, c, dst, sem, device):
        return pltpu.make_async_remote_copy(
            src_ref=snd.at[slot, c], dst_ref=dst, send_sem=send_sem.at[slot], recv_sem=sem,
            device_id={"dp": device}, device_id_type=MESH_ID,
        )

    def to_x(k, c):
        return push(2 * k + OTHER, c, xr.at[k, c], x_sem.at[k, c], x_dev)

    def to_z(slot, box, c):
        return push(slot, c, zr.at[box, c], z_sem.at[box, c], z_dev)

    def to_a(k, c):
        return push(2 * k + MINE, c, ar.at[3 - k, c], a_sem.at[3 - k, c], a_dev)

    def to_tail(c):
        return push(2, c, tr.at[c - tail], t_sem.at[c - tail], z_dev)

    def from_tail(c):
        to_tail(c).wait_recv()
        return tr[c - tail]

    def from_x(k, c):
        to_x(k, c).wait_recv()
        return xr[k, c]

    def from_z(box, c):
        to_z(0, box, c).wait_recv()
        return zr[box, c]

    def from_a(box, c):
        to_a(3 - box, c).wait_recv()
        return ar[box, c]

    def each(low, high, step):
        def one(c, carry):
            step(c)
            return carry

        lax.fori_loop(low, high, one, 0)

    def x_own(k, c):
        snd[2 * k + OTHER, c] = own(2 * k + OTHER, c)
        to_x(k, c).start()

    def share_stats(i):
        return pltpu.make_async_remote_copy(
            src_ref=st0.at[dp], dst_ref=st0.at[dp], send_sem=st0_send.at[i], recv_sem=st0_recv.at[dp],
            device_id={"dp": lax.rem(dp + i, 8)}, device_id_type=MESH_ID,
        )

    def stats_arrival(i):
        peer = lax.rem(dp + i, 8)
        return pltpu.make_async_remote_copy(
            src_ref=st0.at[dp], dst_ref=st0.at[peer], send_sem=st0_send.at[i], recv_sem=st0_recv.at[peer],
            device_id={"dp": peer}, device_id_type=MESH_ID,
        )

    @pl.when(place == 0)
    def _():
        def z_raw(c):
            snd[3, c] = own(3, c)
            to_z(3, 0, c).start()

        def first(c):
            x_own(3, c)
            pl.when(c < early)(lambda: z_raw(c))

        load_head(0).wait()
        x_own(3, 0)
        load_head(1).wait()
        z_raw(0)
        each(1, HEAD, first)
        load_body(0).wait()
        load_body(1).wait()
        each(HEAD, per_layer, first)
        load(7, 1).wait()
        load(3, 1).wait()
        each(per_layer, pieces, first)
        meet()
        for copy in state():
            copy.start()
        loaded(1, 6, 5)
        set_stats()
        for i in range(1, 8):
            share_stats(i).start()

        def second(c):
            snd[6, c] = own(6, c) + from_x(3, c)
            to_z(6, 3, c).start()
            x_own(2, c)

        each(0, pieces, second)
        loaded(4, 2, 0)

        def send_own_level(c):
            snd[1, c] = own(1, c) + from_z(1, c)
            to_x(0, c).start()

        def third(c):
            snd[4, c] = own(4, c) + from_x(2, c)
            to_z(4, 2, c).start()

        def third_a(c):
            third(c)
            x_own(1, c + early)

        def third_b(c):
            third(c)
            send_own_level(c - (pieces - early))

        each(0, pieces - early, third_a)
        each(pieces - early, pieces, third_b)

        def fourth(c):
            snd[2, c] = own(2, c) + from_x(1, c)
            to_z(2, 1, c).start()
            send_own_level(c)

        each(early, pieces, fourth)

        def fifth(c):
            snd[2, c] = own(2, c)
            to_z(2, 1, c).start()

        each(0, tail, fifth)

    @pl.when(place == 1)
    def _():
        load_head(0).wait()
        load_head(1).wait()

        def first(c):
            x_own(3, c)
            snd[1, c] = own(1, c)
            to_z(1, 1, c).start()

        each(0, HEAD, first)
        load_body(0).wait()
        load_body(1).wait()
        each(HEAD, per_layer, first)
        load(7, 1).wait()
        load(1, 1).wait()
        each(per_layer, pieces, first)
        meet()
        for copy in state():
            copy.start()
        loaded(3, 6, 5)
        set_stats()
        for i in range(1, 8):
            share_stats(i).start()
        loaded(4, 2, 0)

        def pass_out(c):
            snd[0, c] = own(0, c) + from_a(0, c)
            to_z(0, 0, c).start()

        def second(c):
            x_own(2, c)

            @pl.when(c < early)
            def _():
                snd[3, c] = own(3, c) + from_z(0, c)
                to_x(1, c).start()

            snd[6, c] = own(6, c) + from_x(3, c) + from_z(3, c)
            to_a(3, c).start()

        def second_b(c):
            second(c)
            pass_out(c - LAG)

        each(0, LAG, second)
        each(LAG, pieces, second_b)

        def third(c):
            @pl.when(c < pieces - early)
            def _():
                x_own(1, c + early)

            snd[4, c] = own(4, c) + from_x(2, c) + from_z(2, c)
            to_a(2, c).start()

            @pl.when(c < LAG)
            def _():
                pass_out(c + pieces - LAG)

        def return_tail(c):
            snd[2, c] = own(2, c) + from_x(1, c) + from_a(1, c)
            to_tail(c).start()

        def third_b(c):
            third(c)
            return_tail(c - LAG)

        each(0, tail + LAG, third)
        each(tail + LAG, early + LAG, third_b)
        each(early + LAG, pieces, third)

    for copy in state():
        copy.wait()

    def weigh(ref, layer, c, factor):
        window = (layer, pl.ds(pl.multiple_of(c * depth, depth), depth))
        ref[window] = ref[window] * factor

    for layer in range(layers):
        def weigh_all(c, layer=layer):
            weigh(params_out, layer, c, 1.0 - learn_rate * decay_rate)
            weigh(moment_out, layer, c, beta_one)
            weigh(second_out, layer, c, beta_two)

        each(0, per_layer, weigh_all)

    for i in range(1, 8):
        stats_arrival(i).wait_recv()
    total = st0[0]
    for i in range(1, 8):
        total = total + st0[i]
    stats_out[...] = total
    weight_sum = weights[0].astype(jnp.float32)
    for layer in range(1, layers):
        weight_sum = weight_sum + weights[layer].astype(jnp.float32)
    square[...] = jnp.zeros_like(square)
    for layer in range(layers):
        factor = weights[layer].astype(jnp.float32) / (weight_sum * total[:, layer : layer + 1])
        factors[layer] = jnp.broadcast_to(factor, factors.shape[1:])

    def count(gradient):
        squares = gradient * gradient
        square[...] += jnp.sum(squares.reshape(depth // 8, 8, squares.shape[1]), axis=0)

    def finish(c, summed):
        layer, r = c // per_layer, lax.rem(c, per_layer)
        gradient = summed * factors[layer]
        out[layer, pl.ds(pl.multiple_of(r * depth, depth), depth), :] = gradient
        return gradient

    def last(c):
        count(finish(c, own(2, c) + from_x(1, c) + from_a(1, c) + from_z(1, c)))

    def finish_tail(c):
        finish(c, snd[2, c] + from_z(1, c))

    def last_end(c):
        count(finish(c, own(0, c) + from_z(0, c) + from_x(0, c)))

    def count_tail(c):
        snd[2, c] = own(2, c)
        count((snd[2, c] + from_tail(c)) * factors[c // per_layer])

    def paced(c):
        to_z(2, 1, c - start + tail).start()
        last_end(c)

    @pl.when(place == 0)
    def _():
        each(tail, early, count_tail)
        each(0, start, last_end)
        each(start, start + paced_pieces, paced)
        each(start + paced_pieces, pieces, last_end)

    @pl.when(place == 1)
    def _():
        each(early, pieces, last)
        each(0, tail, last)

    def share_square(i):
        return pltpu.make_async_remote_copy(
            src_ref=st1.at[place_in_all], dst_ref=st1.at[place_in_all],
            send_sem=st1_send.at[i], recv_sem=st1_recv.at[place_in_all],
            device_id=away(i)[1], device_id_type=MESH_ID,
        )

    def square_arrival(i):
        peer, device = away(i)
        return pltpu.make_async_remote_copy(
            src_ref=st1.at[place_in_all], dst_ref=st1.at[peer], send_sem=st1_send.at[i], recv_sem=st1_recv.at[peer],
            device_id=device, device_id_type=MESH_ID,
        )

    folded = jnp.sum(square[...], axis=0, keepdims=True)
    st1[place_in_all] = sum(folded[:, i : i + LANES] for i in range(0, folded.shape[1], LANES))
    for i in range(devices - 1, 0, -1):
        share_square(i).start()

    @pl.when(place == 0)
    def _():
        each(tail + paced_pieces, early, lambda c: to_z(2, 1, c).start())

    for i in range(1, 8):
        share_stats(i).wait_send()
    for i in range(1, devices):
        share_square(i).wait_send()

    def sent(slot, size=pieces):
        pltpu.make_async_remote_copy(
            src_ref=snd.at[slot, pl.ds(0, size)], dst_ref=zr.at[0, pl.ds(0, size)],
            send_sem=send_sem.at[slot], recv_sem=z_sem.at[0, 0],
            device_id={"dp": z_dev}, device_id_type=MESH_ID,
        ).wait_send()

    for slot in (1, 3, 4, 5, 6, 7):
        sent(slot)

    @pl.when(place == 0)
    def _():
        sent(2)

    @pl.when(place == 1)
    def _():
        sent(0)
        sent(2, TAIL)

    for i in range(1, devices):
        square_arrival(i).wait_recv()
    square_sum = jnp.sum(jnp.sum(st1[...], axis=0), keepdims=True)
    rms_value = jnp.sqrt(square_sum / entries)
    clip_out[...] = jnp.broadcast_to(jnp.minimum(1.0, max_rms / (rms_value + eps_norm)), clip_out.shape)

    @pl.when(place == 1)
    def _():
        each(tail, early, finish_tail)


def update_kernel(gradient, params, moment, second, stats, clip, params_out, moment_out, second_out, mean_out, news, mean, sem, mean_sem):
    layers, rows = gradient.shape[0], gradient.shape[1]
    outs = (params_out, moment_out, second_out)
    chunk, step = min(CHUNK, rows), min(STEP, rows)
    mean[...] = stats[:, layers : 2 * layers] / stats[:, :layers]
    mean_copy = pltpu.make_async_copy(mean, mean_out, mean_sem)
    mean_copy.start()
    clip_scale = clip[...]
    first_scale = (1.0 - beta_one) * clip_scale
    second_scale = (1.0 - beta_two) * clip_scale * clip_scale

    def put(i, layer, low):
        window = (layer, pl.ds(low, chunk))
        return pltpu.make_async_copy(news.at[(i, *window)], outs[i].at[window], sem.at[i])

    chunks = [(layer, low) for layer in range(layers) for low in range(0, rows, chunk)]
    for layer, low in chunks:
        for start in range(low, low + chunk, step):
            window = (layer, pl.ds(start, step))
            held = gradient[window]
            new_moment = moment[window] + first_scale * held
            new_second = second[window] + second_scale * (held * held)
            root = new_second * lax.rsqrt(new_second)
            news[(0, *window)] = params[window] - learn_rate * (new_moment / (root + eps_adam))
            news[(1, *window)] = new_moment
            news[(2, *window)] = new_second
        for i in range(3):
            put(i, layer, low).start()
    for i in range(3):
        pltpu.make_async_copy(news.at[i], outs[i], sem.at[i]).wait()
    mean_copy.wait()


def line_body(n_mp, entries, gradients, layer_mask, exit_losses, exit_weights, params, moment, second):
    layers, rows, columns = params.shape
    depth = min(ROWS, rows)
    pieces = layers * (rows // depth)
    vmem, hbm = pl.BlockSpec(memory_space=pltpu.VMEM), pl.BlockSpec(memory_space=pltpu.HBM)
    block = (pieces, depth, columns)
    f32, dma, regular = jnp.float32, pltpu.SemaphoreType.DMA, pltpu.SemaphoreType.REGULAR
    state = jax.ShapeDtypeStruct((layers, rows, columns), f32)

    def kernel(*refs):
        pl.run_scoped(lambda *sems: line_kernel(n_mp, entries, *refs, *sems),
            dma((3,)), dma((2,)), dma((8, layers)), dma((3,)), dma((8,)), dma((4, pieces)), dma((4, pieces)), dma((2, pieces)), dma((TAIL,)),
            dma((8,)), dma((8,)), dma((8 * n_mp,)), dma((8 * n_mp,)), regular, regular, regular, regular, regular,
        )

    *held, stats, clip = pl.pallas_call(
        kernel,
        name="line_reduce",
        out_shape=(
            state, state, state, state,
            jax.ShapeDtypeStruct((1, LANES), f32),
            jax.ShapeDtypeStruct((1, columns), f32),
        ),
        in_specs=[hbm] * 7,
        out_specs=[vmem] * 6,
        scratch_shapes=[
            pltpu.SMEM(layer_mask.shape, layer_mask.dtype),
            pltpu.SMEM(exit_losses.shape, exit_losses.dtype),
            pltpu.SMEM(exit_weights.shape, exit_weights.dtype),
            pltpu.VMEM((8, layers, rows, columns), gradients.dtype),
            pltpu.VMEM((8, *block), f32),
            pltpu.VMEM((4, *block), f32),
            pltpu.VMEM((4, *block), f32),
            pltpu.VMEM((2, *block), f32),
            pltpu.VMEM((TAIL, *block[1:]), f32),
            pltpu.VMEM((8, 1, LANES), f32),
            pltpu.VMEM((8 * n_mp, 1, LANES), f32),
            pltpu.VMEM((8, columns), f32),
            pltpu.VMEM((layers, 1, columns), f32),
        ],
        compiler_params=pltpu.CompilerParams(
            collective_id=0, has_side_effects=True, vmem_limit_bytes=40 * 1024 * 1024
        ),
    )(*(
        pltpu.with_memory_space_constraint(a, pltpu.HBM)
        for a in (layer_mask, exit_losses, exit_weights, gradients, params, moment, second)
    ))
    *new, mean = pl.pallas_call(
        update_kernel,
        name="update",
        out_shape=(state, state, state, jax.ShapeDtypeStruct((1, layers), f32)),
        in_specs=[vmem] * 6,
        out_specs=[hbm] * 4,
        scratch_shapes=[pltpu.VMEM((3, layers, rows, columns), f32), pltpu.VMEM((1, layers), f32), dma((3,)), dma],
        compiler_params=pltpu.CompilerParams(vmem_limit_bytes=16 * 1024 * 1024),
    )(*held, stats, clip)
    return (*new, mean[0])


def solution(mesh):
    state = P(None, "dp", "mp")
    placed = (P("dp", None, None, "mp"), P("dp", None), P("dp", None), P(), state, state, state)
    n_dp, n_mp = mesh.shape["dp"], mesh.shape["mp"]

    def whole(*args):
        entries = args[4].size
        layers = args[4].shape[0]

        def body(*blocks):
            if n_dp == 8 and n_mp == 4 and layers == 2 and entries == 8 * n_mp * PIECES * ROWS * 256:
                return line_body(n_mp, entries, *blocks)
            return any_mesh_body(entries, *blocks)

        return jax.shard_map(
            body, mesh=mesh, in_specs=placed, out_specs=(state, state, state, P()), check_vma=False
        )(*args)

    return whole
```

```python
import jax
import jax.numpy as jnp
from jax import lax
from jax.experimental import pallas as pl
from jax.experimental.pallas import tpu as pltpu
from jax.sharding import PartitionSpec as P

max_rms = 1.0
eps_norm = 1e-06
eps_adam = 1e-08
beta_one = 0.9
beta_two = 0.95
learn_rate = 0.01
decay_rate = 0.1

MESH_ID = pl.DeviceIdType.MESH
ROWS = 64
LANES = 128
LAG = 4
EARLY = (9, 11)
START = (10, 12)
PACED = (5, 2)
TAIL = 7
GROUP = 4
CHUNK = 64
STEP = 16
MINE, OTHER = 0, 1


def update(gradient, clip_scale, params, moment, second):
    clipped = clip_scale * gradient
    new_moment = beta_one * moment + (1.0 - beta_one) * clipped
    new_second = beta_two * second + (1.0 - beta_two) * clipped * clipped
    new_params = params - learn_rate * (
        new_moment / (jnp.sqrt(new_second) + eps_adam) + decay_rate * params
    )
    return new_params, new_moment, new_second


def any_mesh_body(entries, gradients, layer_mask, exit_losses, exit_weights, params, moment, second):
    keep_float = layer_mask[0].astype(jnp.float32)
    loss_terms = keep_float * exit_losses[0]
    local_term = gradients[0].astype(jnp.float32) * keep_float[:, None, None]
    summed = lax.psum_scatter(local_term, "dp", scatter_dimension=1, tiled=True)
    weight_float = exit_weights.astype(jnp.float32)
    weight_sum = jnp.sum(weight_float)
    layer_count, loss_sum = lax.psum((keep_float, loss_terms), "dp")
    gradient = summed * (weight_float / (weight_sum * layer_count))[:, None, None]
    square_sum = lax.psum(jnp.sum(gradient * gradient), ("dp", "mp"))
    rms_value = jnp.sqrt(square_sum / entries)
    clip_scale = jnp.minimum(1.0, max_rms / (rms_value + eps_norm))
    new = update(gradient, clip_scale, params, moment, second)
    return (*new, loss_sum / layer_count)


def line_kernel(
    n_mp, entries, mask_in, losses_in, weights_in, grads, params_in, moment_in, second_in,
    out, params_out, moment_out, second_out, stats_out, clip_out,
    mask, losses, weights, held, snd, xr, zr, ar, tr, st0, st1, square, factors,
    small_sem, head_sem, load_sem, state_sem, send_sem, xg_sem, zg_sem, x_sem, z_sem, a_sem,
    st0_send, st0_recv, st1_send, st1_recv, end_in, core_in, y_in, middle_in, all_in,
):
    layers, rows = out.shape[0], out.shape[1]
    pieces = snd.shape[1]
    depth = snd.shape[2]
    per_layer = pieces // layers
    dp, mp = lax.axis_index("dp"), lax.axis_index("mp")
    z, x = dp // 2, lax.rem(dp, 2)
    upper = z // 2
    place = lax.rem(z + upper, 2)

    def by_half(pair):
        return pair[0] + upper * (pair[1] - pair[0])

    early, start, paced_pieces = by_half(EARLY), by_half(START), by_half(PACED)
    tail = early - TAIL
    x_dev = z * 2 + 1 - x
    z_dev = (z + 1 - 2 * lax.rem(z, 2)) * 2 + x
    a_dev = (3 - z) * 2 + x

    barrier = pltpu.get_barrier_semaphore()
    devices = 8 * n_mp
    place_in_all = dp * n_mp + mp

    def away(i):
        other_z, other_x, other_mp = z ^ (i // (2 * n_mp)), x ^ (i // n_mp % 2), mp ^ (i % n_mp)
        other_dp = other_z * 2 + other_x
        return other_dp * n_mp + other_mp, {"dp": other_dp, "mp": other_mp}

    def greet(sem, device):
        pl.semaphore_signal(sem, inc=1, device_id=device, device_id_type=MESH_ID)

    for device in ({"dp": x_dev}, {"dp": z_dev}):
        greet(barrier, device)

    @pl.when(place == 1)
    def _():
        for device in ({"dp": a_dev}, {"mp": mp ^ 1}, {"mp": mp ^ 2}):
            greet(barrier, device)

    def load(slot, layer, low=0, high=rows, sem=None):
        k, side = slot // 2, slot % 2
        target = (k + upper * (3 - 2 * k)) * 2 + x + side * (1 - 2 * x)
        return pltpu.make_async_copy(
            grads.at[0, layer, pl.ds(target * rows + low, high - low), :],
            held.at[slot, layer, pl.ds(low, high - low)],
            load_sem.at[slot] if sem is None else head_sem.at[sem],
        )

    def load_head(i):
        return load((7, raw)[i], 0, 0, GROUP * depth, i)

    def load_body(i):
        return load((7, raw)[i], 0, GROUP * depth, rows, 2 + i)

    def load_slot(slot):
        k, side = slot // 2, slot % 2
        target = (k + upper * (3 - 2 * k)) * 2 + x + side * (1 - 2 * x)
        return pltpu.make_async_copy(grads.at[0, :, pl.ds(target * rows, rows), :], held.at[slot], load_sem.at[slot])

    raw = 3 - 2 * place
    small = [
        pltpu.make_async_copy(src, dst, small_sem.at[i])
        for i, (src, dst) in enumerate(((mask_in, mask), (losses_in, losses), (weights_in, weights)))
    ]
    for copy in small:
        copy.start()
    load_head(0).start()
    load_head(1).start()

    load_body(0).start()
    load_body(1).start()

    def fetch(*slots):
        for slot in slots:
            load_slot(slot).start()

    def state():
        pairs = ((params_in, params_out), (moment_in, moment_out), (second_in, second_out))
        return [pltpu.make_async_copy(src, dst, state_sem.at[i]) for i, (src, dst) in enumerate(pairs)]

    load(7, 1).start()
    load(raw, 1).start()
    fetch(6, 5, 4 - raw, 4, 2, 0)

    def loaded(*slots):
        for slot in slots:
            load_slot(slot).wait()

    for copy in small:
        copy.wait()
    lane = lax.broadcasted_iota(jnp.int32, st0.shape[1:], 1)
    tile = jnp.zeros(st0.shape[1:], jnp.float32)
    for layer in range(layers):
        keep = mask[0, layer].astype(jnp.float32)
        tile = jnp.where(lane == layer, keep, tile)
        tile = jnp.where(lane == layers + layer, keep * losses[0, layer], tile)
    st0[dp] = tile

    pl.when(place == 0)(lambda: pl.semaphore_wait(barrier, 2))
    pl.when(place == 1)(lambda: pl.semaphore_wait(barrier, 5))

    def meet():
        @pl.when(place == 0)
        def _():
            greet(end_in, {"dp": z_dev})
            pl.semaphore_wait(all_in, 1)

        @pl.when(place == 1)
        def _():
            pl.semaphore_wait(end_in, 1)
            greet(core_in, {"mp": mp ^ 1})
            pl.semaphore_wait(core_in, 1)
            greet(y_in, {"mp": mp ^ 2})
            pl.semaphore_wait(y_in, 1)
            greet(middle_in, {"dp": a_dev})
            pl.semaphore_wait(middle_in, 1)
            greet(all_in, {"dp": z_dev})

    def own(slot, c):
        layer, r = c // per_layer, lax.rem(c, per_layer)
        keep = mask[0, layer].astype(jnp.float32)
        return held[slot, layer, pl.ds(pl.multiple_of(r * depth, depth), depth), :].astype(jnp.float32) * keep

    def push(slot, c, dst, sem, device, count=None):
        return pltpu.make_async_remote_copy(
            src_ref=snd.at[slot, c if count is None else pl.ds(c, count)], dst_ref=dst, send_sem=send_sem.at[slot], recv_sem=sem,
            device_id={"dp": device}, device_id_type=MESH_ID,
        )

    def to_x(k, c):
        return push(2 * k + OTHER, c, xr.at[k, c], x_sem.at[k, c], x_dev)

    def to_z(slot, box, c):
        return push(slot, c, zr.at[box, c], z_sem.at[box, c], z_dev)

    def group_to_x(k, c):
        return push(2 * k + OTHER, c, xr.at[k, pl.ds(c, GROUP)], xg_sem.at[k - 2, c // GROUP], x_dev, GROUP)

    def group_to_z(k, c):
        return push(2 * k + MINE, c, zr.at[k, pl.ds(c, GROUP)], zg_sem.at[k - 2, c // GROUP], z_dev, GROUP)

    def to_a(k, c):
        return push(2 * k + MINE, c, ar.at[3 - k, c], a_sem.at[3 - k, c], a_dev)

    def to_tail(c):
        return push(2, c, tr.at[c - tail], a_sem.at[0, c - tail], z_dev)

    def from_tail(c):
        to_tail(c).wait_recv()
        return tr[c - tail]

    def from_x(k, c):
        to_x(k, c).wait_recv()
        return xr[k, c]

    def from_z(box, c):
        to_z(0, box, c).wait_recv()
        return zr[box, c]

    def from_a(box, c):
        to_a(3 - box, c).wait_recv()
        return ar[box, c]

    def each(low, high, step):
        def one(c, carry):
            step(c)
            return carry

        lax.fori_loop(low, high, one, 0)

    def x_own(k, c):
        snd[2 * k + OTHER, c] = own(2 * k + OTHER, c)
        to_x(k, c).start()

    def x_group(k, c):
        for i in range(GROUP):
            snd[2 * k + OTHER, c + i] = own(2 * k + OTHER, c + i)
        group_to_x(k, c).start()

    def groups(low, high, step):
        each(low // GROUP, high // GROUP, lambda g: step(g * GROUP))

    def share_stats(i):
        return pltpu.make_async_remote_copy(
            src_ref=st0.at[dp], dst_ref=st0.at[dp], send_sem=st0_send, recv_sem=st0_recv,
            device_id={"dp": lax.rem(dp + i, 8)}, device_id_type=MESH_ID,
        )

    def all_stats():
        return pltpu.make_async_remote_copy(
            src_ref=st0.at[pl.ds(0, 7)], dst_ref=st0.at[pl.ds(0, 7)], send_sem=st0_send, recv_sem=st0_recv,
            device_id={"dp": x_dev}, device_id_type=MESH_ID,
        )

    @pl.when(place == 0)
    def _():
        def z_raw(c):
            snd[3, c] = own(3, c)
            to_z(3, 0, c).start()

        def first(c):
            x_group(3, c)
            for i in range(GROUP):
                pl.when(c + i < early)(lambda: z_raw(c + i))

        load_head(0).wait()
        x_group(3, 0)
        load_head(1).wait()
        for i in range(GROUP):
            z_raw(i)
        load_body(0).wait()
        load_body(1).wait()
        groups(GROUP, per_layer, first)
        load(7, 1).wait()
        load(3, 1).wait()
        groups(per_layer, pieces, first)
        meet()
        for copy in state():
            copy.start()
        loaded(1, 6, 5)
        for i in range(1, 8):
            share_stats(i).start()

        def pass_on(k, c):
            group_to_x(k, c).wait_recv()
            for i in range(GROUP):
                snd[2 * k, c + i] = own(2 * k, c + i) + xr[k, c + i]
            group_to_z(k, c).start()

        def second(c):
            pass_on(3, c)
            x_group(2, c)

        groups(0, pieces, second)
        loaded(4, 2, 0)

        def send_own_level(c):
            snd[1, c] = own(1, c) + from_z(1, c)
            to_x(0, c).start()

        def third(c):
            pass_on(2, c)
            for i in range(GROUP):
                pl.when(c + i < pieces - early)(lambda: x_own(1, c + i + early))
                pl.when(c + i >= pieces - early)(lambda: send_own_level(c + i - (pieces - early)))

        groups(0, pieces, third)

        def fourth(c):
            snd[2, c] = own(2, c) + from_x(1, c)
            to_z(2, 1, c).start()
            send_own_level(c)

        each(early, pieces, fourth)

        def fifth(c):
            snd[2, c] = own(2, c)
            to_z(2, 1, c).start()

        each(0, tail, fifth)

    @pl.when(place == 1)
    def _():
        load_head(0).wait()
        load_head(1).wait()

        def first(c):
            x_group(3, c)
            for i in range(GROUP):
                snd[1, c + i] = own(1, c + i)
                to_z(1, 1, c + i).start()

        groups(0, GROUP, first)
        load_body(0).wait()
        load_body(1).wait()
        groups(GROUP, per_layer, first)
        load(7, 1).wait()
        load(1, 1).wait()
        groups(per_layer, pieces, first)
        meet()
        for copy in state():
            copy.start()
        loaded(3, 6, 5)
        for i in range(1, 8):
            share_stats(i).start()
        loaded(4, 2, 0)

        def pass_out(c):
            snd[0, c] = own(0, c) + from_a(0, c)
            to_z(0, 0, c).start()

        def merge(k, c):
            group_to_x(k, c).wait_recv()
            group_to_z(k, c).wait_recv()
            for i in range(GROUP):
                snd[2 * k, c + i] = own(2 * k, c + i) + xr[k, c + i] + zr[k, c + i]
                to_a(k, c + i).start()

        def x_early(c):
            snd[3, c] = own(3, c) + from_z(0, c)
            to_x(1, c).start()

        def second(c):
            x_group(2, c)
            for i in range(GROUP):
                pl.when(c + i < early)(lambda: x_early(c + i))
            merge(3, c)
            for i in range(GROUP):
                pl.when(c >= LAG)(lambda: pass_out(c + i - LAG))

        groups(0, pieces, second)

        def return_tail(c):
            snd[2, c] = own(2, c) + from_x(1, c) + from_a(1, c)
            to_tail(c).start()

        def third(c):
            for i in range(GROUP):
                pl.when(c + i < pieces - early)(lambda: x_own(1, c + i + early))
            merge(2, c)
            for i in range(GROUP):
                late = c + i - LAG
                pl.when(c < LAG)(lambda: pass_out(late + pieces))
                pl.when((late >= tail) & (late < early))(lambda: return_tail(late))

        groups(0, pieces, third)

    for copy in state():
        copy.wait()

    def weigh(ref, layer, c, factor):
        window = (layer, pl.ds(pl.multiple_of(c * depth, depth), depth))
        ref[window] = ref[window] * factor

    for layer in range(layers):
        def weigh_all(c, layer=layer):
            weigh(params_out, layer, c, 1.0 - learn_rate * decay_rate)
            weigh(moment_out, layer, c, beta_one)
            weigh(second_out, layer, c, beta_two)

        each(0, per_layer, weigh_all)

    all_stats().wait_recv()
    total = st0[0]
    for i in range(1, 8):
        total = total + st0[i]
    stats_out[...] = total
    weight_sum = weights[0].astype(jnp.float32)
    for layer in range(1, layers):
        weight_sum = weight_sum + weights[layer].astype(jnp.float32)
    square[...] = jnp.zeros_like(square)
    for layer in range(layers):
        factor = weights[layer].astype(jnp.float32) / (weight_sum * total[:, layer : layer + 1])
        factors[layer] = jnp.broadcast_to(factor, factors.shape[1:])

    def count(gradient):
        squares = gradient * gradient
        square[...] += jnp.sum(squares.reshape(depth // 8, 8, squares.shape[1]), axis=0)

    def finish(c, summed):
        layer, r = c // per_layer, lax.rem(c, per_layer)
        gradient = summed * factors[layer]
        out[layer, pl.ds(pl.multiple_of(r * depth, depth), depth), :] = gradient
        return gradient

    def last(c):
        count(finish(c, own(2, c) + from_x(1, c) + from_a(1, c) + from_z(1, c)))

    def finish_tail(c):
        finish(c, snd[2, c] + from_z(1, c))

    def last_end(c):
        count(finish(c, own(0, c) + from_z(0, c) + from_x(0, c)))

    def count_tail(c):
        snd[2, c] = own(2, c)
        count((snd[2, c] + from_tail(c)) * factors[c // per_layer])

    def paced(c):
        to_z(2, 1, c - start + tail).start()
        last_end(c)

    @pl.when(place == 0)
    def _():
        each(tail, early, count_tail)
        each(0, start, last_end)
        each(start, start + paced_pieces, paced)
        each(start + paced_pieces, pieces, last_end)

    @pl.when(place == 1)
    def _():
        each(early, pieces, last)
        each(0, tail, last)

    def share_square(i):
        return pltpu.make_async_remote_copy(
            src_ref=st1.at[place_in_all], dst_ref=st1.at[place_in_all],
            send_sem=st1_send, recv_sem=st1_recv,
            device_id=away(i)[1], device_id_type=MESH_ID,
        )

    def all_squares():
        return pltpu.make_async_remote_copy(
            src_ref=st1.at[pl.ds(0, devices - 1)], dst_ref=st1.at[pl.ds(0, devices - 1)],
            send_sem=st1_send, recv_sem=st1_recv, device_id={"dp": x_dev}, device_id_type=MESH_ID,
        )

    folded = jnp.sum(square[...], axis=0, keepdims=True)
    st1[place_in_all] = sum(folded[:, i : i + LANES] for i in range(0, folded.shape[1], LANES))
    for i in range(devices - 1, 0, -1):
        share_square(i).start()

    @pl.when(place == 0)
    def _():
        each(tail + paced_pieces, early, lambda c: to_z(2, 1, c).start())

    all_stats().wait_send()
    all_squares().wait_send()

    def sent(slot, size=pieces):
        pltpu.make_async_remote_copy(
            src_ref=snd.at[slot, pl.ds(0, size)], dst_ref=zr.at[0, pl.ds(0, size)],
            send_sem=send_sem.at[slot], recv_sem=z_sem.at[0, 0],
            device_id={"dp": z_dev}, device_id_type=MESH_ID,
        ).wait_send()

    for slot in (1, 3, 4, 5, 6, 7):
        sent(slot)

    @pl.when(place == 0)
    def _():
        sent(2)

    @pl.when(place == 1)
    def _():
        sent(0)
        sent(2, TAIL)

    all_squares().wait_recv()
    square_sum = jnp.sum(jnp.sum(st1[...], axis=0), keepdims=True)
    rms_value = jnp.sqrt(square_sum / entries)
    clip_out[...] = jnp.broadcast_to(jnp.minimum(1.0, max_rms / (rms_value + eps_norm)), clip_out.shape)

    @pl.when(place == 1)
    def _():
        each(tail, early, finish_tail)


def update_kernel(gradient, params, moment, second, stats, clip, params_out, moment_out, second_out, mean_out, news, mean, sem, mean_sem):
    layers, rows = gradient.shape[0], gradient.shape[1]
    outs = (params_out, moment_out, second_out)
    chunk, step = min(CHUNK, rows), min(STEP, rows)
    mean[...] = stats[:, layers : 2 * layers] / stats[:, :layers]
    mean_copy = pltpu.make_async_copy(mean, mean_out, mean_sem)
    mean_copy.start()
    clip_scale = clip[...]
    first_scale = (1.0 - beta_one) * clip_scale
    second_scale = (1.0 - beta_two) * clip_scale * clip_scale

    def put(i, layer, low):
        window = (layer, pl.ds(low, chunk))
        return pltpu.make_async_copy(news.at[(i, *window)], outs[i].at[window], sem.at[i])

    chunks = [(layer, low) for layer in range(layers) for low in range(0, rows, chunk)]
    for layer, low in chunks:
        for start in range(low, low + chunk, step):
            window = (layer, pl.ds(start, step))
            held = gradient[window]
            new_moment = moment[window] + first_scale * held
            new_second = second[window] + second_scale * (held * held)
            root = new_second * lax.rsqrt(new_second)
            news[(0, *window)] = params[window] - learn_rate * (new_moment / (root + eps_adam))
            news[(1, *window)] = new_moment
            news[(2, *window)] = new_second
        for i in range(3):
            put(i, layer, low).start()
    for i in range(3):
        pltpu.make_async_copy(news.at[i], outs[i], sem.at[i]).wait()
    mean_copy.wait()


def line_body(n_mp, entries, gradients, layer_mask, exit_losses, exit_weights, params, moment, second):
    layers, rows, columns = params.shape
    depth = min(ROWS, rows)
    pieces = layers * (rows // depth)
    vmem, hbm = pl.BlockSpec(memory_space=pltpu.VMEM), pl.BlockSpec(memory_space=pltpu.HBM)
    block = (pieces, depth, columns)
    f32, dma, regular = jnp.float32, pltpu.SemaphoreType.DMA, pltpu.SemaphoreType.REGULAR
    state = jax.ShapeDtypeStruct((layers, rows, columns), f32)

    def kernel(*refs):
        line_kernel(n_mp, entries, *refs)

    *held, stats, clip = pl.pallas_call(
        kernel,
        name="line_reduce",
        out_shape=(
            state, state, state, state,
            jax.ShapeDtypeStruct((1, LANES), f32),
            jax.ShapeDtypeStruct((1, columns), f32),
        ),
        in_specs=[hbm] * 7,
        out_specs=[vmem] * 6,
        scratch_shapes=[
            pltpu.SMEM(layer_mask.shape, layer_mask.dtype),
            pltpu.SMEM(exit_losses.shape, exit_losses.dtype),
            pltpu.SMEM(exit_weights.shape, exit_weights.dtype),
            pltpu.VMEM((8, layers, rows, columns), gradients.dtype),
            pltpu.VMEM((8, *block), f32),
            pltpu.VMEM((4, *block), f32),
            pltpu.VMEM((4, *block), f32),
            pltpu.VMEM((2, *block), f32),
            pltpu.VMEM((TAIL, *block[1:]), f32),
            pltpu.VMEM((8, 1, LANES), f32),
            pltpu.VMEM((8 * n_mp, 1, LANES), f32),
            pltpu.VMEM((8, columns), f32),
            pltpu.VMEM((layers, 1, columns), f32),
            dma((3,)), dma((4,)), dma((8,)), dma((3,)), dma((8,)), dma((2, pieces // GROUP)), dma((2, pieces // GROUP)),
            dma((2, pieces)), dma((2, pieces)), dma((2, pieces)), dma, dma, dma, dma,
            regular, regular, regular, regular, regular,
        ],
        compiler_params=pltpu.CompilerParams(
            collective_id=0, has_side_effects=True, vmem_limit_bytes=40 * 1024 * 1024
        ),
    )(*(
        pltpu.with_memory_space_constraint(a, pltpu.HBM)
        for a in (layer_mask, exit_losses, exit_weights, gradients, params, moment, second)
    ))
    *new, mean = pl.pallas_call(
        update_kernel,
        name="update",
        out_shape=(state, state, state, jax.ShapeDtypeStruct((1, layers), f32)),
        in_specs=[vmem] * 6,
        out_specs=[hbm] * 4,
        scratch_shapes=[pltpu.VMEM((3, layers, rows, columns), f32), pltpu.VMEM((1, layers), f32), dma((3,)), dma],
        compiler_params=pltpu.CompilerParams(vmem_limit_bytes=16 * 1024 * 1024),
    )(*held, stats, clip)
    return (*new, mean[0])


def solution(mesh):
    state = P(None, "dp", "mp")
    placed = (P("dp", None, None, "mp"), P("dp", None), P("dp", None), P(), state, state, state)
    n_dp, n_mp = mesh.shape["dp"], mesh.shape["mp"]

    def whole(*args):
        entries = args[4].size
        layers = args[4].shape[0]

        def body(*blocks):
            if n_dp == 8 and n_mp == 4 and layers == 2:
                return line_body(n_mp, entries, *blocks)
            return any_mesh_body(entries, *blocks)

        return jax.shard_map(
            body, mesh=mesh, in_specs=placed, out_specs=(state, state, state, P()), check_vma=False
        )(*args)

    return whole
```

```python
import jax
import jax.numpy as jnp
from jax import lax
from jax.experimental import pallas as pl
from jax.experimental.pallas import tpu as pltpu
from jax.sharding import PartitionSpec as P

max_rms = 1.0
eps_norm = 1e-06
eps_adam = 1e-08
beta_one = 0.9
beta_two = 0.95
learn_rate = 0.01
decay_rate = 0.1

MESH_ID = pl.DeviceIdType.MESH
ROWS = 32
PIECES = 32
LANES = 128
LAG = 8
EARLY = (18, 21)
START = (19, 25)
PACED = (10, 4)
TAIL = 12
HEAD = 2
CHUNK = 64
STEP = 16
MINE, OTHER = 0, 1


def update(gradient, clip_scale, params, moment, second):
    clipped = clip_scale * gradient
    new_moment = beta_one * moment + (1.0 - beta_one) * clipped
    new_second = beta_two * second + (1.0 - beta_two) * clipped * clipped
    new_params = params - learn_rate * (
        new_moment / (jnp.sqrt(new_second) + eps_adam) + decay_rate * params
    )
    return new_params, new_moment, new_second


def any_mesh_body(entries, gradients, layer_mask, exit_losses, exit_weights, params, moment, second):
    keep_float = layer_mask[0].astype(jnp.float32)
    loss_terms = keep_float * exit_losses[0]
    local_term = gradients[0].astype(jnp.float32) * keep_float[:, None, None]
    summed = lax.psum_scatter(local_term, "dp", scatter_dimension=1, tiled=True)
    weight_float = exit_weights.astype(jnp.float32)
    weight_sum = jnp.sum(weight_float)
    layer_count, loss_sum = lax.psum((keep_float, loss_terms), "dp")
    gradient = summed * (weight_float / (weight_sum * layer_count))[:, None, None]
    square_sum = lax.psum(jnp.sum(gradient * gradient), ("dp", "mp"))
    rms_value = jnp.sqrt(square_sum / entries)
    clip_scale = jnp.minimum(1.0, max_rms / (rms_value + eps_norm))
    new = update(gradient, clip_scale, params, moment, second)
    return (*new, loss_sum / layer_count)


def line_kernel(
    n_mp, entries, mask_in, losses_in, weights_in, grads, params_in, moment_in, second_in,
    out, params_out, moment_out, second_out, stats_out, clip_out,
    mask, losses, weights, held, snd, xr, zr, ar, tr, st0, st1, square, factors,
    small_sem, head_sem, load_sem, state_sem, send_sem, x_sem, z_sem, a_sem, t_sem,
    st0_send, st0_recv, st1_send, st1_recv, end_in, core_in, y_in, middle_in, all_in,
):
    layers, rows = out.shape[0], out.shape[1]
    pieces = snd.shape[1]
    depth = snd.shape[2]
    per_layer = pieces // layers
    dp, mp = lax.axis_index("dp"), lax.axis_index("mp")
    z, x = dp // 2, lax.rem(dp, 2)
    upper = z // 2
    place = lax.rem(z + upper, 2)

    def by_half(pair):
        return pair[0] + upper * (pair[1] - pair[0])

    early, start, paced_pieces = by_half(EARLY), by_half(START), by_half(PACED)
    tail = early - TAIL
    x_dev = z * 2 + 1 - x
    z_dev = (z + 1 - 2 * lax.rem(z, 2)) * 2 + x
    a_dev = (3 - z) * 2 + x

    barrier = pltpu.get_barrier_semaphore()
    devices = 8 * n_mp
    place_in_all = dp * n_mp + mp

    def away(i):
        other_z, other_x, other_mp = z ^ (i // (2 * n_mp)), x ^ (i // n_mp % 2), mp ^ (i % n_mp)
        other_dp = other_z * 2 + other_x
        return other_dp * n_mp + other_mp, {"dp": other_dp, "mp": other_mp}

    def greet(sem, device):
        pl.semaphore_signal(sem, inc=1, device_id=device, device_id_type=MESH_ID)

    def load(slot, layer, low=0, high=rows, sem=None):
        k, side = slot // 2, slot % 2
        target = (k + upper * (3 - 2 * k)) * 2 + x + side * (1 - 2 * x)
        return pltpu.make_async_copy(
            grads.at[0, layer, pl.ds(target * rows + low, high - low), :],
            held.at[slot, layer, pl.ds(low, high - low)],
            load_sem.at[slot, layer] if sem is None else head_sem.at[sem],
        )

    def load_head(i):
        return load((7, raw)[i], 0, 0, HEAD * depth, i)

    def load_body(i):
        return load((7, raw)[i], 0, HEAD * depth)

    raw = 3 - 2 * place
    small = [
        pltpu.make_async_copy(src, dst, small_sem.at[i])
        for i, (src, dst) in enumerate(((mask_in, mask), (losses_in, losses), (weights_in, weights)))
    ]
    small[0].start()
    load_head(0).start()
    load_head(1).start()
    greet(barrier, {"dp": x_dev})
    greet(barrier, {"dp": z_dev})

    @pl.when(place == 1)
    def _():
        for device in ({"dp": a_dev}, {"mp": mp ^ 1}, {"mp": mp ^ 2}):
            greet(barrier, device)

    load_body(0).start()
    load_body(1).start()

    def fetch(*slots):
        for slot in slots:
            for layer in range(layers):
                load(slot, layer).start()

    def state():
        pairs = ((params_in, params_out), (moment_in, moment_out), (second_in, second_out))
        return [pltpu.make_async_copy(src, dst, state_sem.at[i]) for i, (src, dst) in enumerate(pairs)]

    load(7, 1).start()
    load(raw, 1).start()
    fetch(6, 5, 4 - raw, 4, 2, 0)
    for copy in small[1:]:
        copy.start()

    def loaded(*slots):
        for slot in slots:
            for layer in range(layers):
                load(slot, layer).wait()

    small[0].wait()
    pl.when(place == 0)(lambda: pl.semaphore_wait(barrier, 2))
    pl.when(place == 1)(lambda: pl.semaphore_wait(barrier, 5))

    def set_stats():
        for copy in small[1:]:
            copy.wait()
        lane = lax.broadcasted_iota(jnp.int32, st0.shape[1:], 1)
        tile = jnp.zeros(st0.shape[1:], jnp.float32)
        for layer in range(layers):
            keep = mask[0, layer].astype(jnp.float32)
            tile = jnp.where(lane == layer, keep, tile)
            tile = jnp.where(lane == layers + layer, keep * losses[0, layer], tile)
        st0[dp] = tile

    def meet():
        @pl.when(place == 0)
        def _():
            greet(end_in, {"dp": z_dev})
            pl.semaphore_wait(all_in, 1)

        @pl.when(place == 1)
        def _():
            pl.semaphore_wait(end_in, 1)
            greet(core_in, {"mp": mp ^ 1})
            pl.semaphore_wait(core_in, 1)
            greet(y_in, {"mp": mp ^ 2})
            pl.semaphore_wait(y_in, 1)
            greet(middle_in, {"dp": a_dev})
            pl.semaphore_wait(middle_in, 1)
            greet(all_in, {"dp": z_dev})

    def own(slot, c):
        layer, r = c // per_layer, lax.rem(c, per_layer)
        keep = mask[0, layer].astype(jnp.float32)
        return held[slot, layer, pl.ds(pl.multiple_of(r * depth, depth), depth), :].astype(jnp.float32) * keep

    def push(slot, c, dst, sem, device):
        return pltpu.make_async_remote_copy(
            src_ref=snd.at[slot, c], dst_ref=dst, send_sem=send_sem.at[slot], recv_sem=sem,
            device_id={"dp": device}, device_id_type=MESH_ID,
        )

    def to_x(k, c):
        return push(2 * k + OTHER, c, xr.at[k, c], x_sem.at[k, c], x_dev)

    def to_z(slot, box, c):
        return push(slot, c, zr.at[box, c], z_sem.at[box, c], z_dev)

    def to_a(k, c):
        return push(2 * k + MINE, c, ar.at[3 - k, c], a_sem.at[3 - k, c], a_dev)

    def to_tail(c):
        return push(2, c, tr.at[c - tail], t_sem.at[c - tail], z_dev)

    def from_tail(c):
        to_tail(c).wait_recv()
        return tr[c - tail]

    def from_x(k, c):
        to_x(k, c).wait_recv()
        return xr[k, c]

    def from_z(box, c):
        to_z(0, box, c).wait_recv()
        return zr[box, c]

    def from_a(box, c):
        to_a(3 - box, c).wait_recv()
        return ar[box, c]

    def each(low, high, step):
        def one(c, carry):
            step(c)
            return carry

        lax.fori_loop(low, high, one, 0)

    def x_own(k, c):
        snd[2 * k + OTHER, c] = own(2 * k + OTHER, c)
        to_x(k, c).start()

    def share_stats(i):
        return pltpu.make_async_remote_copy(
            src_ref=st0.at[dp], dst_ref=st0.at[dp], send_sem=st0_send.at[i], recv_sem=st0_recv.at[dp],
            device_id={"dp": lax.rem(dp + i, 8)}, device_id_type=MESH_ID,
        )

    def stats_arrival(i):
        peer = lax.rem(dp + i, 8)
        return pltpu.make_async_remote_copy(
            src_ref=st0.at[dp], dst_ref=st0.at[peer], send_sem=st0_send.at[i], recv_sem=st0_recv.at[peer],
            device_id={"dp": peer}, device_id_type=MESH_ID,
        )

    @pl.when(place == 0)
    def _():
        def z_raw(c):
            snd[3, c] = own(3, c)
            to_z(3, 0, c).start()

        def first(c):
            x_own(3, c)
            pl.when(c < early)(lambda: z_raw(c))

        load_head(0).wait()
        x_own(3, 0)
        load_head(1).wait()
        z_raw(0)
        each(1, HEAD, first)
        load_body(0).wait()
        load_body(1).wait()
        each(HEAD, per_layer, first)
        load(7, 1).wait()
        load(3, 1).wait()
        each(per_layer, pieces, first)
        meet()
        for copy in state():
            copy.start()
        loaded(1, 6, 5)
        set_stats()
        for i in range(1, 8):
            share_stats(i).start()

        def second(c):
            snd[6, c] = own(6, c) + from_x(3, c)
            to_z(6, 3, c).start()
            x_own(2, c)

        each(0, pieces, second)
        loaded(4, 2, 0)

        def send_own_level(c):
            snd[1, c] = own(1, c) + from_z(1, c)
            to_x(0, c).start()

        def third(c):
            snd[4, c] = own(4, c) + from_x(2, c)
            to_z(4, 2, c).start()

        def third_a(c):
            third(c)
            x_own(1, c + early)

        def third_b(c):
            third(c)
            send_own_level(c - (pieces - early))

        each(0, pieces - early, third_a)
        each(pieces - early, pieces, third_b)

        def fourth(c):
            snd[2, c] = own(2, c) + from_x(1, c)
            to_z(2, 1, c).start()
            send_own_level(c)

        each(early, pieces, fourth)

        def fifth(c):
            snd[2, c] = own(2, c)
            to_z(2, 1, c).start()

        each(0, tail, fifth)

    @pl.when(place == 1)
    def _():
        load_head(0).wait()
        load_head(1).wait()

        def first(c):
            x_own(3, c)
            snd[1, c] = own(1, c)
            to_z(1, 1, c).start()

        each(0, HEAD, first)
        load_body(0).wait()
        load_body(1).wait()
        each(HEAD, per_layer, first)
        load(7, 1).wait()
        load(1, 1).wait()
        each(per_layer, pieces, first)
        meet()
        for copy in state():
            copy.start()
        loaded(3, 6, 5)
        set_stats()
        for i in range(1, 8):
            share_stats(i).start()
        loaded(4, 2, 0)

        def pass_out(c):
            snd[0, c] = own(0, c) + from_a(0, c)
            to_z(0, 0, c).start()

        def second(c):
            x_own(2, c)

            @pl.when(c < early)
            def _():
                snd[3, c] = own(3, c) + from_z(0, c)
                to_x(1, c).start()

            snd[6, c] = own(6, c) + from_x(3, c) + from_z(3, c)
            to_a(3, c).start()

        def second_b(c):
            second(c)
            pass_out(c - LAG)

        each(0, LAG, second)
        each(LAG, pieces, second_b)

        def third(c):
            @pl.when(c < pieces - early)
            def _():
                x_own(1, c + early)

            snd[4, c] = own(4, c) + from_x(2, c) + from_z(2, c)
            to_a(2, c).start()

            @pl.when(c < LAG)
            def _():
                pass_out(c + pieces - LAG)

        def return_tail(c):
            snd[2, c] = own(2, c) + from_x(1, c) + from_a(1, c)
            to_tail(c).start()

        def third_b(c):
            third(c)
            return_tail(c - LAG)

        each(0, tail + LAG, third)
        each(tail + LAG, early + LAG, third_b)
        each(early + LAG, pieces, third)

    for copy in state():
        copy.wait()

    def weigh(ref, layer, c, factor):
        window = (layer, pl.ds(pl.multiple_of(c * depth, depth), depth))
        ref[window] = ref[window] * factor

    for layer in range(layers):
        def weigh_all(c, layer=layer):
            weigh(params_out, layer, c, 1.0 - learn_rate * decay_rate)
            weigh(moment_out, layer, c, beta_one)
            weigh(second_out, layer, c, beta_two)

        each(0, per_layer, weigh_all)

    for i in range(1, 8):
        stats_arrival(i).wait_recv()
    total = st0[0]
    for i in range(1, 8):
        total = total + st0[i]
    stats_out[...] = total
    weight_sum = weights[0].astype(jnp.float32)
    for layer in range(1, layers):
        weight_sum = weight_sum + weights[layer].astype(jnp.float32)
    square[...] = jnp.zeros_like(square)
    for layer in range(layers):
        factor = weights[layer].astype(jnp.float32) / (weight_sum * total[:, layer : layer + 1])
        factors[layer] = jnp.broadcast_to(factor, factors.shape[1:])

    def count(gradient):
        squares = gradient * gradient
        square[...] += jnp.sum(squares.reshape(depth // 8, 8, squares.shape[1]), axis=0)

    def finish(c, summed):
        layer, r = c // per_layer, lax.rem(c, per_layer)
        gradient = summed * factors[layer]
        out[layer, pl.ds(pl.multiple_of(r * depth, depth), depth), :] = gradient
        return gradient

    def last(c):
        count(finish(c, own(2, c) + from_x(1, c) + from_a(1, c) + from_z(1, c)))

    def finish_tail(c):
        finish(c, snd[2, c] + from_z(1, c))

    def last_end(c):
        count(finish(c, own(0, c) + from_z(0, c) + from_x(0, c)))

    def count_tail(c):
        snd[2, c] = own(2, c)
        count((snd[2, c] + from_tail(c)) * factors[c // per_layer])

    def paced(c):
        to_z(2, 1, c - start + tail).start()
        last_end(c)

    @pl.when(place == 0)
    def _():
        each(tail, early, count_tail)
        each(0, start, last_end)
        each(start, start + paced_pieces, paced)
        each(start + paced_pieces, pieces, last_end)

    @pl.when(place == 1)
    def _():
        each(early, pieces, last)
        each(0, tail, last)

    def share_square(i):
        return pltpu.make_async_remote_copy(
            src_ref=st1.at[place_in_all], dst_ref=st1.at[place_in_all],
            send_sem=st1_send, recv_sem=st1_recv,
            device_id=away(i)[1], device_id_type=MESH_ID,
        )

    def all_squares():
        return pltpu.make_async_remote_copy(
            src_ref=st1.at[pl.ds(0, devices - 1)], dst_ref=st1.at[pl.ds(0, devices - 1)],
            send_sem=st1_send, recv_sem=st1_recv, device_id={"dp": x_dev}, device_id_type=MESH_ID,
        )

    folded = jnp.sum(square[...], axis=0, keepdims=True)
    st1[place_in_all] = sum(folded[:, i : i + LANES] for i in range(0, folded.shape[1], LANES))
    for i in range(devices - 1, 0, -1):
        share_square(i).start()

    @pl.when(place == 0)
    def _():
        each(tail + paced_pieces, early, lambda c: to_z(2, 1, c).start())

    for i in range(1, 8):
        share_stats(i).wait_send()
    all_squares().wait_send()

    def sent(slot, size=pieces):
        pltpu.make_async_remote_copy(
            src_ref=snd.at[slot, pl.ds(0, size)], dst_ref=zr.at[0, pl.ds(0, size)],
            send_sem=send_sem.at[slot], recv_sem=z_sem.at[0, 0],
            device_id={"dp": z_dev}, device_id_type=MESH_ID,
        ).wait_send()

    for slot in (1, 3, 4, 5, 6, 7):
        sent(slot)

    @pl.when(place == 0)
    def _():
        sent(2)

    @pl.when(place == 1)
    def _():
        sent(0)
        sent(2, TAIL)

    all_squares().wait_recv()
    square_sum = jnp.sum(jnp.sum(st1[...], axis=0), keepdims=True)
    rms_value = jnp.sqrt(square_sum / entries)
    clip_out[...] = jnp.broadcast_to(jnp.minimum(1.0, max_rms / (rms_value + eps_norm)), clip_out.shape)

    @pl.when(place == 1)
    def _():
        each(tail, early, finish_tail)


def update_kernel(gradient, params, moment, second, stats, clip, params_out, moment_out, second_out, mean_out, news, mean, sem, mean_sem):
    layers, rows = gradient.shape[0], gradient.shape[1]
    outs = (params_out, moment_out, second_out)
    chunk, step = min(CHUNK, rows), min(STEP, rows)
    mean[...] = stats[:, layers : 2 * layers] / stats[:, :layers]
    mean_copy = pltpu.make_async_copy(mean, mean_out, mean_sem)
    mean_copy.start()
    clip_scale = clip[...]
    first_scale = (1.0 - beta_one) * clip_scale
    second_scale = (1.0 - beta_two) * clip_scale * clip_scale

    def put(i, layer, low):
        window = (layer, pl.ds(low, chunk))
        return pltpu.make_async_copy(news.at[(i, *window)], outs[i].at[window], sem.at[i])

    chunks = [(layer, low) for layer in range(layers) for low in range(0, rows, chunk)]
    for layer, low in chunks:
        for start in range(low, low + chunk, step):
            window = (layer, pl.ds(start, step))
            held = gradient[window]
            new_moment = moment[window] + first_scale * held
            new_second = second[window] + second_scale * (held * held)
            root = new_second * lax.rsqrt(new_second)
            news[(0, *window)] = params[window] - learn_rate * (new_moment / (root + eps_adam))
            news[(1, *window)] = new_moment
            news[(2, *window)] = new_second
        for i in range(3):
            put(i, layer, low).start()
    for i in range(3):
        pltpu.make_async_copy(news.at[i], outs[i], sem.at[i]).wait()
    mean_copy.wait()


def line_body(n_mp, entries, gradients, layer_mask, exit_losses, exit_weights, params, moment, second):
    layers, rows, columns = params.shape
    depth = min(ROWS, rows)
    pieces = layers * (rows // depth)
    vmem, hbm = pl.BlockSpec(memory_space=pltpu.VMEM), pl.BlockSpec(memory_space=pltpu.HBM)
    block = (pieces, depth, columns)
    f32, dma, regular = jnp.float32, pltpu.SemaphoreType.DMA, pltpu.SemaphoreType.REGULAR
    state = jax.ShapeDtypeStruct((layers, rows, columns), f32)

    def kernel(*refs):
        pl.run_scoped(lambda *sems: line_kernel(n_mp, entries, *refs, *sems),
            dma((3,)), dma((2,)), dma((8, layers)), dma((3,)), dma((8,)), dma((4, pieces)), dma((4, pieces)), dma((2, pieces)), dma((TAIL,)),
            dma((8,)), dma((8,)), dma, dma, regular, regular, regular, regular, regular,
        )

    *held, stats, clip = pl.pallas_call(
        kernel,
        name="line_reduce",
        out_shape=(
            state, state, state, state,
            jax.ShapeDtypeStruct((1, LANES), f32),
            jax.ShapeDtypeStruct((1, columns), f32),
        ),
        in_specs=[hbm] * 7,
        out_specs=[vmem] * 6,
        scratch_shapes=[
            pltpu.SMEM(layer_mask.shape, layer_mask.dtype),
            pltpu.SMEM(exit_losses.shape, exit_losses.dtype),
            pltpu.SMEM(exit_weights.shape, exit_weights.dtype),
            pltpu.VMEM((8, layers, rows, columns), gradients.dtype),
            pltpu.VMEM((8, *block), f32),
            pltpu.VMEM((4, *block), f32),
            pltpu.VMEM((4, *block), f32),
            pltpu.VMEM((2, *block), f32),
            pltpu.VMEM((TAIL, *block[1:]), f32),
            pltpu.VMEM((8, 1, LANES), f32),
            pltpu.VMEM((8 * n_mp, 1, LANES), f32),
            pltpu.VMEM((8, columns), f32),
            pltpu.VMEM((layers, 1, columns), f32),
        ],
        compiler_params=pltpu.CompilerParams(
            collective_id=0, has_side_effects=True, vmem_limit_bytes=40 * 1024 * 1024
        ),
    )(*(
        pltpu.with_memory_space_constraint(a, pltpu.HBM)
        for a in (layer_mask, exit_losses, exit_weights, gradients, params, moment, second)
    ))
    *new, mean = pl.pallas_call(
        update_kernel,
        name="update",
        out_shape=(state, state, state, jax.ShapeDtypeStruct((1, layers), f32)),
        in_specs=[vmem] * 6,
        out_specs=[hbm] * 4,
        scratch_shapes=[pltpu.VMEM((3, layers, rows, columns), f32), pltpu.VMEM((1, layers), f32), dma((3,)), dma],
        compiler_params=pltpu.CompilerParams(vmem_limit_bytes=16 * 1024 * 1024),
    )(*held, stats, clip)
    return (*new, mean[0])


def solution(mesh):
    state = P(None, "dp", "mp")
    placed = (P("dp", None, None, "mp"), P("dp", None), P("dp", None), P(), state, state, state)
    n_dp, n_mp = mesh.shape["dp"], mesh.shape["mp"]

    def whole(*args):
        entries = args[4].size
        layers = args[4].shape[0]

        def body(*blocks):
            if n_dp == 8 and n_mp == 4 and layers == 2 and entries == 8 * n_mp * PIECES * ROWS * 256:
                return line_body(n_mp, entries, *blocks)
            return any_mesh_body(entries, *blocks)

        return jax.shard_map(
            body, mesh=mesh, in_specs=placed, out_specs=(state, state, state, P()), check_vma=False
        )(*args)

    return whole
```

```python
import jax
import jax.numpy as jnp
from jax import lax
from jax.experimental import pallas as pl
from jax.experimental.pallas import tpu as pltpu
from jax.sharding import PartitionSpec as P

max_rms = 1.0
eps_norm = 1e-06
eps_adam = 1e-08
beta_one = 0.9
beta_two = 0.95
learn_rate = 0.01
decay_rate = 0.1

MESH_ID = pl.DeviceIdType.MESH
ROWS = 32
PIECES = 32
LANES = 128
LAG = 8
EARLY = (18, 21)
START = (19, 25)
PACED = (10, 4)
TAIL = 12
HEAD = 2
CHUNK = 64
STEP = 16
MINE, OTHER = 0, 1


def update(gradient, clip_scale, params, moment, second):
    clipped = clip_scale * gradient
    new_moment = beta_one * moment + (1.0 - beta_one) * clipped
    new_second = beta_two * second + (1.0 - beta_two) * clipped * clipped
    new_params = params - learn_rate * (
        new_moment / (jnp.sqrt(new_second) + eps_adam) + decay_rate * params
    )
    return new_params, new_moment, new_second


def any_mesh_body(entries, gradients, layer_mask, exit_losses, exit_weights, params, moment, second):
    keep_float = layer_mask[0].astype(jnp.float32)
    loss_terms = keep_float * exit_losses[0]
    local_term = gradients[0].astype(jnp.float32) * keep_float[:, None, None]
    summed = lax.psum_scatter(local_term, "dp", scatter_dimension=1, tiled=True)
    weight_float = exit_weights.astype(jnp.float32)
    weight_sum = jnp.sum(weight_float)
    layer_count, loss_sum = lax.psum((keep_float, loss_terms), "dp")
    gradient = summed * (weight_float / (weight_sum * layer_count))[:, None, None]
    square_sum = lax.psum(jnp.sum(gradient * gradient), ("dp", "mp"))
    rms_value = jnp.sqrt(square_sum / entries)
    clip_scale = jnp.minimum(1.0, max_rms / (rms_value + eps_norm))
    new = update(gradient, clip_scale, params, moment, second)
    return (*new, loss_sum / layer_count)


def line_kernel(
    n_mp, entries, mask_in, losses_in, weights_in, grads, params_in, moment_in, second_in,
    out, params_out, moment_out, second_out, stats_out, clip_out,
    mask, losses, weights, held, snd, xr, zr, ar, tr, st0, st1, square, factors,
    small_sem, head_sem, load_sem, state_sem, send_sem, x_sem, z_sem, a_sem, t_sem,
    st0_send, st0_recv, st1_send, st1_recv, end_in, core_in, y_in, middle_in, all_in,
):
    layers, rows = out.shape[0], out.shape[1]
    pieces = snd.shape[1]
    depth = snd.shape[2]
    per_layer = pieces // layers
    dp, mp = lax.axis_index("dp"), lax.axis_index("mp")
    z, x = dp // 2, lax.rem(dp, 2)
    upper = z // 2
    place = lax.rem(z + upper, 2)

    def by_half(pair):
        return pair[0] + upper * (pair[1] - pair[0])

    early, start, paced_pieces = by_half(EARLY), by_half(START), by_half(PACED)
    tail = early - TAIL
    x_dev = z * 2 + 1 - x
    z_dev = (z + 1 - 2 * lax.rem(z, 2)) * 2 + x
    a_dev = (3 - z) * 2 + x

    barrier = pltpu.get_barrier_semaphore()
    devices = 8 * n_mp
    place_in_all = dp * n_mp + mp

    def greet(sem, device):
        pl.semaphore_signal(sem, inc=1, device_id=device, device_id_type=MESH_ID)

    def load(slot, layer, low=0, high=rows, sem=None):
        k, side = slot // 2, slot % 2
        target = (k + upper * (3 - 2 * k)) * 2 + x + side * (1 - 2 * x)
        return pltpu.make_async_copy(
            grads.at[0, layer, pl.ds(target * rows + low, high - low), :],
            held.at[slot, layer, pl.ds(low, high - low)],
            load_sem.at[slot, layer] if sem is None else head_sem.at[sem],
        )

    def load_head(i):
        return load((7, raw)[i], 0, 0, HEAD * depth, i)

    def load_body(i):
        return load((7, raw)[i], 0, HEAD * depth)

    raw = 3 - 2 * place
    small = [
        pltpu.make_async_copy(src, dst, small_sem.at[i])
        for i, (src, dst) in enumerate(((mask_in, mask), (losses_in, losses), (weights_in, weights)))
    ]
    small[0].start()
    load_head(0).start()
    load_head(1).start()
    greet(barrier, {"dp": x_dev})
    greet(barrier, {"dp": z_dev})

    @pl.when(place == 1)
    def _():
        for device in ({"dp": a_dev}, {"mp": mp ^ 1}, {"mp": mp ^ 2}):
            greet(barrier, device)

    load_body(0).start()
    load_body(1).start()

    def fetch(*slots):
        for slot in slots:
            for layer in range(layers):
                load(slot, layer).start()

    def state():
        pairs = ((params_in, params_out), (moment_in, moment_out), (second_in, second_out))
        return [pltpu.make_async_copy(src, dst, state_sem.at[i]) for i, (src, dst) in enumerate(pairs)]

    load(7, 1).start()
    load(raw, 1).start()
    fetch(6, 5, 4 - raw, 4, 2, 0)
    for copy in small[1:]:
        copy.start()

    def loaded(*slots):
        for slot in slots:
            for layer in range(layers):
                load(slot, layer).wait()

    small[0].wait()
    pl.when(place == 0)(lambda: pl.semaphore_wait(barrier, 2))
    pl.when(place == 1)(lambda: pl.semaphore_wait(barrier, 5))

    def set_stats():
        for copy in small[1:]:
            copy.wait()
        lane = lax.broadcasted_iota(jnp.int32, st0.shape[1:], 1)
        tile = jnp.zeros(st0.shape[1:], jnp.float32)
        for layer in range(layers):
            keep = mask[0, layer].astype(jnp.float32)
            tile = jnp.where(lane == layer, keep, tile)
            tile = jnp.where(lane == layers + layer, keep * losses[0, layer], tile)
        st0[dp] = tile

    def meet():
        @pl.when(place == 0)
        def _():
            greet(end_in, {"dp": z_dev})
            pl.semaphore_wait(all_in, 1)

        @pl.when(place == 1)
        def _():
            pl.semaphore_wait(end_in, 1)
            greet(core_in, {"mp": mp ^ 1})
            pl.semaphore_wait(core_in, 1)
            greet(y_in, {"mp": mp ^ 2})
            pl.semaphore_wait(y_in, 1)
            greet(middle_in, {"dp": a_dev})
            pl.semaphore_wait(middle_in, 1)
            greet(all_in, {"dp": z_dev})

    def own(slot, c):
        layer, r = c // per_layer, lax.rem(c, per_layer)
        keep = mask[0, layer].astype(jnp.float32)
        return held[slot, layer, pl.ds(pl.multiple_of(r * depth, depth), depth), :].astype(jnp.float32) * keep

    def push(slot, c, dst, sem, device):
        return pltpu.make_async_remote_copy(
            src_ref=snd.at[slot, c], dst_ref=dst, send_sem=send_sem.at[slot], recv_sem=sem,
            device_id={"dp": device}, device_id_type=MESH_ID,
        )

    def to_x(k, c):
        return push(2 * k + OTHER, c, xr.at[k, c], x_sem.at[k, c], x_dev)

    def to_z(slot, box, c):
        return push(slot, c, zr.at[box, c], z_sem.at[box, c], z_dev)

    def to_a(k, c):
        return push(2 * k + MINE, c, ar.at[3 - k, c], a_sem.at[3 - k, c], a_dev)

    def to_tail(c):
        return push(2, c, tr.at[c - tail], t_sem.at[c - tail], z_dev)

    def from_tail(c):
        to_tail(c).wait_recv()
        return tr[c - tail]

    def from_x(k, c):
        to_x(k, c).wait_recv()
        return xr[k, c]

    def from_z(box, c):
        to_z(0, box, c).wait_recv()
        return zr[box, c]

    def from_a(box, c):
        to_a(3 - box, c).wait_recv()
        return ar[box, c]

    def each(low, high, step):
        def one(c, carry):
            step(c)
            return carry

        lax.fori_loop(low, high, one, 0)

    def x_own(k, c):
        snd[2 * k + OTHER, c] = own(2 * k + OTHER, c)
        to_x(k, c).start()

    def share_stats(i):
        return pltpu.make_async_remote_copy(
            src_ref=st0.at[dp], dst_ref=st0.at[dp], send_sem=st0_send.at[i], recv_sem=st0_recv.at[dp],
            device_id={"dp": lax.rem(dp + i, 8)}, device_id_type=MESH_ID,
        )

    def stats_arrival(i):
        peer = lax.rem(dp + i, 8)
        return pltpu.make_async_remote_copy(
            src_ref=st0.at[dp], dst_ref=st0.at[peer], send_sem=st0_send.at[i], recv_sem=st0_recv.at[peer],
            device_id={"dp": peer}, device_id_type=MESH_ID,
        )

    @pl.when(place == 0)
    def _():
        def z_raw(c):
            snd[3, c] = own(3, c)
            to_z(3, 0, c).start()

        def first(c):
            x_own(3, c)
            pl.when(c < early)(lambda: z_raw(c))

        load_head(0).wait()
        x_own(3, 0)
        load_head(1).wait()
        z_raw(0)
        each(1, HEAD, first)
        load_body(0).wait()
        load_body(1).wait()
        each(HEAD, per_layer, first)
        load(7, 1).wait()
        load(3, 1).wait()
        each(per_layer, pieces, first)
        meet()
        for copy in state():
            copy.start()
        loaded(1, 6, 5)
        set_stats()
        for i in range(1, 8):
            share_stats(i).start()

        def second(c):
            snd[6, c] = own(6, c) + from_x(3, c)
            to_z(6, 3, c).start()
            x_own(2, c)

        each(0, pieces, second)
        loaded(4, 2, 0)

        def send_own_level(c):
            snd[1, c] = own(1, c) + from_z(1, c)
            to_x(0, c).start()

        def third(c):
            snd[4, c] = own(4, c) + from_x(2, c)
            to_z(4, 2, c).start()

        def third_a(c):
            third(c)
            x_own(1, c + early)

        def third_b(c):
            third(c)
            send_own_level(c - (pieces - early))

        each(0, pieces - early, third_a)
        each(pieces - early, pieces, third_b)

        def fourth(c):
            snd[2, c] = own(2, c) + from_x(1, c)
            to_z(2, 1, c).start()
            send_own_level(c)

        each(early, pieces, fourth)

        def fifth(c):
            snd[2, c] = own(2, c)
            to_z(2, 1, c).start()

        each(0, tail, fifth)

    @pl.when(place == 1)
    def _():
        load_head(0).wait()
        load_head(1).wait()

        def first(c):
            x_own(3, c)
            snd[1, c] = own(1, c)
            to_z(1, 1, c).start()

        each(0, HEAD, first)
        load_body(0).wait()
        load_body(1).wait()
        each(HEAD, per_layer, first)
        load(7, 1).wait()
        load(1, 1).wait()
        each(per_layer, pieces, first)
        meet()
        for copy in state():
            copy.start()
        loaded(3, 6, 5)
        set_stats()
        for i in range(1, 8):
            share_stats(i).start()
        loaded(4, 2, 0)

        def pass_out(c):
            snd[0, c] = own(0, c) + from_a(0, c)
            to_z(0, 0, c).start()

        def second(c):
            x_own(2, c)

            @pl.when(c < early)
            def _():
                snd[3, c] = own(3, c) + from_z(0, c)
                to_x(1, c).start()

            snd[6, c] = own(6, c) + from_x(3, c) + from_z(3, c)
            to_a(3, c).start()

        def second_b(c):
            second(c)
            pass_out(c - LAG)

        each(0, LAG, second)
        each(LAG, pieces, second_b)

        def third(c):
            @pl.when(c < pieces - early)
            def _():
                x_own(1, c + early)

            snd[4, c] = own(4, c) + from_x(2, c) + from_z(2, c)
            to_a(2, c).start()

            @pl.when(c < LAG)
            def _():
                pass_out(c + pieces - LAG)

        def return_tail(c):
            snd[2, c] = own(2, c) + from_x(1, c) + from_a(1, c)
            to_tail(c).start()

        def third_b(c):
            third(c)
            return_tail(c - LAG)

        each(0, tail + LAG, third)
        each(tail + LAG, early + LAG, third_b)
        each(early + LAG, pieces, third)

    for copy in state():
        copy.wait()

    def weigh(ref, layer, c, factor):
        window = (layer, pl.ds(pl.multiple_of(c * depth, depth), depth))
        ref[window] = ref[window] * factor

    for layer in range(layers):
        def weigh_all(c, layer=layer):
            weigh(params_out, layer, c, 1.0 - learn_rate * decay_rate)
            weigh(moment_out, layer, c, beta_one)
            weigh(second_out, layer, c, beta_two)

        each(0, per_layer, weigh_all)

    for i in range(1, 8):
        stats_arrival(i).wait_recv()
    total = st0[0]
    for i in range(1, 8):
        total = total + st0[i]
    stats_out[...] = total
    weight_sum = weights[0].astype(jnp.float32)
    for layer in range(1, layers):
        weight_sum = weight_sum + weights[layer].astype(jnp.float32)
    square[...] = jnp.zeros_like(square)
    for layer in range(layers):
        factor = weights[layer].astype(jnp.float32) / (weight_sum * total[:, layer : layer + 1])
        factors[layer] = jnp.broadcast_to(factor, factors.shape[1:])

    def count(gradient):
        squares = gradient * gradient
        square[...] += jnp.sum(squares.reshape(depth // 8, 8, squares.shape[1]), axis=0)

    def finish(c, summed):
        layer, r = c // per_layer, lax.rem(c, per_layer)
        gradient = summed * factors[layer]
        out[layer, pl.ds(pl.multiple_of(r * depth, depth), depth), :] = gradient
        return gradient

    def last(c):
        count(finish(c, own(2, c) + from_x(1, c) + from_a(1, c) + from_z(1, c)))

    def finish_tail(c):
        finish(c, snd[2, c] + from_z(1, c))

    def last_end(c):
        count(finish(c, own(0, c) + from_z(0, c) + from_x(0, c)))

    def count_tail(c):
        snd[2, c] = own(2, c)
        count((snd[2, c] + from_tail(c)) * factors[c // per_layer])

    def paced(c):
        to_z(2, 1, c - start + tail).start()
        last_end(c)

    @pl.when(place == 0)
    def _():
        each(tail, early, count_tail)
        each(0, start, last_end)
        each(start, start + paced_pieces, paced)
        each(start + paced_pieces, pieces, last_end)

    @pl.when(place == 1)
    def _():
        each(early, pieces, last)
        each(0, tail, last)

    def share_square(target):
        return pltpu.make_async_remote_copy(
            src_ref=st1.at[place_in_all], dst_ref=st1.at[place_in_all], send_sem=st1_send, recv_sem=st1_recv,
            device_id={"dp": target // n_mp, "mp": target % n_mp}, device_id_type=MESH_ID,
        )

    def all_squares():
        return pltpu.make_async_remote_copy(
            src_ref=st1.at[pl.ds(0, devices - 1)], dst_ref=st1.at[pl.ds(0, devices - 1)],
            send_sem=st1_send, recv_sem=st1_recv, device_id={"dp": x_dev}, device_id_type=MESH_ID,
        )

    folded = jnp.sum(square[...], axis=0, keepdims=True)
    st1[place_in_all] = sum(folded[:, i : i + LANES] for i in range(0, folded.shape[1], LANES))
    for target in range(devices):
        pl.when(place_in_all != target)(lambda: share_square(target).start())

    @pl.when(place == 0)
    def _():
        each(tail + paced_pieces, early, lambda c: to_z(2, 1, c).start())

    for i in range(1, 8):
        share_stats(i).wait_send()
    all_squares().wait_send()

    def sent(slot, size=pieces):
        pltpu.make_async_remote_copy(
            src_ref=snd.at[slot, pl.ds(0, size)], dst_ref=zr.at[0, pl.ds(0, size)],
            send_sem=send_sem.at[slot], recv_sem=z_sem.at[0, 0],
            device_id={"dp": z_dev}, device_id_type=MESH_ID,
        ).wait_send()

    for slot in (1, 3, 4, 5, 6, 7):
        sent(slot)

    @pl.when(place == 0)
    def _():
        sent(2)

    @pl.when(place == 1)
    def _():
        sent(0)
        sent(2, TAIL)

    all_squares().wait_recv()
    square_sum = jnp.sum(jnp.sum(st1[...], axis=0), keepdims=True)
    rms_value = jnp.sqrt(square_sum / entries)
    clip_out[...] = jnp.broadcast_to(jnp.minimum(1.0, max_rms / (rms_value + eps_norm)), clip_out.shape)

    @pl.when(place == 1)
    def _():
        each(tail, early, finish_tail)


def update_kernel(gradient, params, moment, second, stats, clip, params_out, moment_out, second_out, mean_out, news, mean, sem, mean_sem):
    layers, rows = gradient.shape[0], gradient.shape[1]
    outs = (params_out, moment_out, second_out)
    chunk, step = min(CHUNK, rows), min(STEP, rows)
    mean[...] = stats[:, layers : 2 * layers] / stats[:, :layers]
    mean_copy = pltpu.make_async_copy(mean, mean_out, mean_sem)
    mean_copy.start()
    clip_scale = clip[...]
    first_scale = (1.0 - beta_one) * clip_scale
    second_scale = (1.0 - beta_two) * clip_scale * clip_scale

    def put(i, layer, low):
        window = (layer, pl.ds(low, chunk))
        return pltpu.make_async_copy(news.at[(i, *window)], outs[i].at[window], sem.at[i])

    chunks = [(layer, low) for layer in range(layers) for low in range(0, rows, chunk)]
    for layer, low in chunks:
        for start in range(low, low + chunk, step):
            window = (layer, pl.ds(start, step))
            held = gradient[window]
            new_moment = moment[window] + first_scale * held
            new_second = second[window] + second_scale * (held * held)
            root = new_second * lax.rsqrt(new_second)
            news[(0, *window)] = params[window] - learn_rate * (new_moment / (root + eps_adam))
            news[(1, *window)] = new_moment
            news[(2, *window)] = new_second
        for i in range(3):
            put(i, layer, low).start()
    for i in range(3):
        pltpu.make_async_copy(news.at[i], outs[i], sem.at[i]).wait()
    mean_copy.wait()


def line_body(n_mp, entries, gradients, layer_mask, exit_losses, exit_weights, params, moment, second):
    layers, rows, columns = params.shape
    depth = min(ROWS, rows)
    pieces = layers * (rows // depth)
    vmem, hbm = pl.BlockSpec(memory_space=pltpu.VMEM), pl.BlockSpec(memory_space=pltpu.HBM)
    block = (pieces, depth, columns)
    f32, dma, regular = jnp.float32, pltpu.SemaphoreType.DMA, pltpu.SemaphoreType.REGULAR
    state = jax.ShapeDtypeStruct((layers, rows, columns), f32)

    def kernel(*refs):
        pl.run_scoped(lambda *sems: line_kernel(n_mp, entries, *refs, *sems),
            dma((3,)), dma((2,)), dma((8, layers)), dma((3,)), dma((8,)), dma((4, pieces)), dma((4, pieces)), dma((2, pieces)), dma((TAIL,)),
            dma((8,)), dma((8,)), dma, dma, regular, regular, regular, regular, regular,
        )

    *held, stats, clip = pl.pallas_call(
        kernel,
        name="line_reduce",
        out_shape=(
            state, state, state, state,
            jax.ShapeDtypeStruct((1, LANES), f32),
            jax.ShapeDtypeStruct((1, columns), f32),
        ),
        in_specs=[hbm] * 7,
        out_specs=[vmem] * 6,
        scratch_shapes=[
            pltpu.SMEM(layer_mask.shape, layer_mask.dtype),
            pltpu.SMEM(exit_losses.shape, exit_losses.dtype),
            pltpu.SMEM(exit_weights.shape, exit_weights.dtype),
            pltpu.VMEM((8, layers, rows, columns), gradients.dtype),
            pltpu.VMEM((8, *block), f32),
            pltpu.VMEM((4, *block), f32),
            pltpu.VMEM((4, *block), f32),
            pltpu.VMEM((2, *block), f32),
            pltpu.VMEM((TAIL, *block[1:]), f32),
            pltpu.VMEM((8, 1, LANES), f32),
            pltpu.VMEM((8 * n_mp, 1, LANES), f32),
            pltpu.VMEM((8, columns), f32),
            pltpu.VMEM((layers, 1, columns), f32),
        ],
        compiler_params=pltpu.CompilerParams(
            collective_id=0, has_side_effects=True, vmem_limit_bytes=40 * 1024 * 1024
        ),
    )(*(
        pltpu.with_memory_space_constraint(a, pltpu.HBM)
        for a in (layer_mask, exit_losses, exit_weights, gradients, params, moment, second)
    ))
    *new, mean = pl.pallas_call(
        update_kernel,
        name="update",
        out_shape=(state, state, state, jax.ShapeDtypeStruct((1, layers), f32)),
        in_specs=[vmem] * 6,
        out_specs=[hbm] * 4,
        scratch_shapes=[pltpu.VMEM((3, layers, rows, columns), f32), pltpu.VMEM((1, layers), f32), dma((3,)), dma],
        compiler_params=pltpu.CompilerParams(vmem_limit_bytes=16 * 1024 * 1024),
    )(*held, stats, clip)
    return (*new, mean[0])


def solution(mesh):
    state = P(None, "dp", "mp")
    placed = (P("dp", None, None, "mp"), P("dp", None), P("dp", None), P(), state, state, state)
    n_dp, n_mp = mesh.shape["dp"], mesh.shape["mp"]

    def whole(*args):
        entries = args[4].size
        layers = args[4].shape[0]

        def body(*blocks):
            if n_dp == 8 and n_mp == 4 and layers == 2 and entries == 8 * n_mp * PIECES * ROWS * 256:
                return line_body(n_mp, entries, *blocks)
            return any_mesh_body(entries, *blocks)

        return jax.shard_map(
            body, mesh=mesh, in_specs=placed, out_specs=(state, state, state, P()), check_vma=False
        )(*args)

    return whole
```
